8 devices in a mesh: rep: 1 (over z), r: 2 (over y), s: 4 (over x, core).
Axes of the slice: x: 2, y: 2, z: 1, core: 2. Of those that a mesh axis runs over, the one named last changes fastest.
Arguments:
- x: bfloat16 [8, 4096, 1280], P(('rep', 'r', 's'))
- dy: bfloat16 [8, 4096, 1280], P(('rep', 'r', 's'))
- w_gate: bfloat16 [2, 1280, 3072], P(None, 's')
- w_up: bfloat16 [2, 1280, 3072], P(None, 's')
- w_down: bfloat16 [2, 3072, 1280], P(None, 's')
Outputs:
- output 1: bfloat16 [8, 4096, 1280], P(('rep', 'r', 's'))
- output 2: bfloat16 [2, 1280, 3072], P('rep', 's')
- output 3: bfloat16 [2, 1280, 3072], P('rep', 's')
- output 4: bfloat16 [2, 3072, 1280], P('rep', 's')
All inputs are finite; a program needn't handle non-finite values.
Results may differ from the reference program's by a relative error of at most 0.018.
Values are sent between devices in bfloat16 or wider.
A program may use at most 2 GiB of HBM per device.

```python
import jax
import jax.numpy as jnp
from jax import lax

SEQUENCES = 8
TOKENS = 4096
D = 1280
FF = 3072
LAYERS = 2
NAMES = ("w_gate", "w_up", "w_down")
SHAPES = {"w_gate": (LAYERS, D, FF), "w_up": (LAYERS, D, FF), "w_down": (LAYERS, FF, D)}


def bump(key, n, height):
    away = (jnp.arange(n, dtype=jnp.int32) - jax.random.randint(key, (), 0, n, jnp.int32)) % n
    return jnp.where(away < n // 8, height, 1.0)


def together(key, own, strength):
    shared = jax.random.normal(key, own.shape[1:], jnp.float32)
    return (own + strength * shared) * lax.rsqrt(1 + strength * strength)


def setup_inputs(seed: int = 0, part: int = 0) -> dict:
    kx, kdy, ka, kb, kz, kf, kh, kl, *kw = jax.random.split(jax.random.key(seed), 8 + len(NAMES))
    kx, kdy, ka, kb = (jax.random.fold_in(k, part) for k in (kx, kdy, ka, kb))
    shape = (SEQUENCES, TOKENS, D)
    much_x, much_dy = jax.random.uniform(kz, (2,), jnp.float32, 0.0, 1.0)
    layers = 2.0 ** jax.random.uniform(kl, (LAYERS, 1, 1), jnp.float32, -1.0, 1.0)
    x = together(ka, jax.random.normal(kx, shape, jnp.float32), much_x) * bump(kf, D, 4.0)
    dy = together(kb, jax.random.normal(kdy, shape, jnp.float32), much_dy)
    drawn = {"x": x.astype(jnp.bfloat16), "dy": (dy * (SEQUENCES * TOKENS) ** -0.5).astype(jnp.bfloat16)}
    for key, name in zip(kw, NAMES, strict=True):
        w = jax.random.normal(key, SHAPES[name], jnp.float32) * SHAPES[name][1] ** -0.5
        drawn[name] = (w * {"w_gate": 1.0, "w_up": bump(kh, FF, 4.0), "w_down": layers}[name]).astype(jnp.bfloat16)
    return drawn


def matmul(a, w):
    return jnp.dot(a, w, preferred_element_type=jnp.float32).astype(jnp.bfloat16)


def normed(h):
    wide = h.astype(jnp.float32)
    scale = lax.rsqrt(jnp.mean(wide**2, -1, keepdims=True) + 1e-6)
    return (wide * scale).astype(jnp.bfloat16)


def layer(h, w):
    a = normed(h)
    gate = jnp.dot(a, w["w_gate"], preferred_element_type=jnp.float32)
    up = jnp.dot(a, w["w_up"], preferred_element_type=jnp.float32)
    return h + matmul((jax.nn.silu(gate) * up).astype(jnp.bfloat16), w["w_down"])


def stack(weights, h):
    return lax.scan(lambda h, w: (layer(h, w), None), h, weights)[0]


def reference(x, dy, w_gate, w_up, w_down):
    weights = dict(zip(NAMES, (w_gate, w_up, w_down), strict=True))

    def take(so_far, sequence):
        h, by_y = sequence
        _, back = jax.vjp(stack, weights, h)
        by_weights, by_h = back(by_y)
        return jax.tree.map(lambda total, term: total + term.astype(jnp.float32), so_far, by_weights), by_h

    none_yet = {name: jnp.zeros(w.shape, jnp.float32) for name, w in weights.items()}
    by_weights, by_x = lax.scan(take, none_yet, (x, dy))
    return (by_x, *(by_weights[name].astype(jnp.bfloat16) for name in NAMES))
```

```python
import jax
import jax.numpy as jnp
from jax import lax
from jax.experimental import pallas as pl
from jax.experimental.pallas import tpu as pltpu
from jax.sharding import PartitionSpec as P

F32, BF16 = jnp.float32, jnp.bfloat16
ANY = pl.BlockSpec(memory_space=pl.ANY)
MESH = pl.DeviceIdType.MESH
NT = (((1,), (1,)), ((), ()))
TN = (((0,), (0,)), ((), ()))
CHUNKS = 4


def dot(a, b):
    return jnp.dot(a, b, preferred_element_type=F32)


def dot_nt(a, b):
    return lax.dot_general(a, b, NT, preferred_element_type=F32)


def dot_tn(a, b):
    return lax.dot_general(a, b, TN, preferred_element_type=F32)


def rounded(v):
    return v.astype(BF16).astype(F32)


def sigmoid(g):
    return pl.reciprocal(1.0 + jnp.exp(-g))


def normed(wide):
    return wide * lax.rsqrt(jnp.mean(wide * wide, -1, keepdims=True) + 1e-6)


def rows(tile, width):
    return pl.BlockSpec((tile, width), lambda i: (i, 0))


def shaped(*shape, dtype=BF16):
    return jax.ShapeDtypeStruct(shape, dtype)


class Place:
    def __init__(self):
        self.me, self.y = lax.axis_index("s"), lax.axis_index("r")
        x, c = self.me // 2, self.me % 2
        self.mate, self.far, self.far_mate = 2 * x + 1 - c, 2 * (1 - x) + c, 2 * (1 - x) + 1 - c
        self.to = {"mate": {"s": self.mate}, "x": {"s": self.far}, "y": {"r": 1 - self.y}}

    def greet(self, whom):
        barrier = pltpu.get_barrier_semaphore()
        for name in whom:
            pl.semaphore_signal(barrier, inc=1, device_id=self.to[name], device_id_type=MESH)
        pl.semaphore_wait(barrier, len(whom))


def part_rows(ref, start, size):
    return ref.at[pl.ds(pl.multiple_of(start, 16), size)]


def params(collective=None):
    more = {} if collective is None else dict(collective_id=collective, has_side_effects=True)
    return pltpu.CompilerParams(dimension_semantics=("arbitrary",), vmem_limit_bytes=62 << 20, **more)


def cost(flops):
    return pl.CostEstimate(flops=flops, bytes_accessed=1 << 20, transcendentals=0)


class Unit:
    def __init__(self, name, layer, start, width):
        self.name, self.layer, self.start, self.width = name, layer, start, width


class Mover:
    KINDS = ("own", "x", "y", "straight", "around")

    def __init__(self, units, weights, buffers, send, recv):
        self.units, self.weights, self.buffers, self.send, self.recv = units, weights, buffers, send, recv
        self.at = Place()

    def copy(self, n, kind, arriving=False):
        unit, buf, at = self.units[n], self.buffers[n], self.at
        block = buf.shape[0] // 4
        half = block // 2
        w = self.weights[unit.name].at[unit.layer]
        cols = pl.ds(unit.start, unit.width)
        mine, other = at.y * half, (1 - at.y) * half
        if arriving:
            start, size = {
                "own": (at.mate * block, block),
                "x": (at.far * block + mine, half),
                "y": (at.far * block + other, half),
                "straight": (at.far_mate * block + mine, half),
                "around": (at.far_mate * block + other, half),
            }[kind]
            src = dst = part_rows(buf, start, size)
        elif kind == "own":
            src, dst = w.at[:, cols], part_rows(buf, at.me * block, block)
        elif kind == "x":
            src, dst = w.at[pl.ds(pl.multiple_of(mine, 16), half), cols], part_rows(buf, at.me * block + mine, half)
        else:
            src = dst = part_rows(buf, at.far * block + (other if kind == "around" else mine), half)
        k = self.KINDS.index(kind)
        to = at.to[{"x": "x", "y": "y"}.get(kind, "mate")]
        return pltpu.make_async_remote_copy(src, dst, self.send.at[n, k], self.recv.at[n, k], device_id=to, device_id_type=MESH)

    def start(self, ns, *kinds):
        for n in ns:
            for kind in kinds:
                self.copy(n, kind).start()

    def arrived(self, ns, *kinds):
        for n in ns:
            for kind in kinds:
                self.copy(n, kind, arriving=True).wait_recv()

    def sent(self, ns):
        for n in ns:
            for kind in self.KINDS:
                self.copy(n, kind).wait_send()


def load(pairs, sems, first=0):
    at, made = Place(), []
    for units, scratch in pairs:
        col = 0
        for unit, w, buf in units:
            block = buf.shape[0] // 4
            for n, who in enumerate((at.me, at.mate, at.far, at.far_mate)):
                src = w.at[unit.layer, :, pl.ds(unit.start, unit.width)] if n == 0 else part_rows(buf, who * block, block)
                dst = scratch.at[pl.ds(pl.multiple_of(who * block, 16), block), pl.ds(col, unit.width)]
                made.append(pltpu.make_async_copy(src, dst, sems.at[first + len(made)]))
                made[-1].start()
            col += unit.width
    return made


class Whole:
    def __init__(self, w, units, buffers):
        self.w, self.units, self.buffers = w, units, buffers
        self.operands = [w, *buffers]
        self.shape = (4 * w.shape[1], w.shape[2])
        self.copies = 4 * len(units)

    def pairs(self, refs):
        return [(unit, refs[0], buf) for unit, buf in zip(self.units, refs[1:], strict=True)]


def fetch(matrices, refs, scratches, sems):
    @pl.when(pl.program_id(0) == 0)
    def _():
        pairs, used = [], 0
        for matrix, scratch in zip(matrices, scratches, strict=True):
            count = len(matrix.operands)
            pairs.append((matrix.pairs(refs[used : used + count]), scratch))
            used += count
        for copy in load(pairs, sems):
            copy.wait()


class Sends:
    def __init__(self, *items):
        self.items = items
        self.arrays = [array for array, _ in items]
        self.out_shape = [shaped(2, array.shape[0] // 4, array.shape[1]) if to == "term" else shaped(*array.shape) for array, to in items]
        self.count = sum(2 if to == "term" else 1 for _, to in items)
        self.scratch = [pltpu.SemaphoreType.DMA((self.count,))] * 2 if items else []
        self.whom = sorted({"mate" if to == "term" else to for _, to in items})

    def copies(self, at, sources, targets, send, recv):
        made = []
        for (array, to), src, dst in zip(self.items, sources, targets, strict=True):
            pairs = [(src, dst)]
            if to == "term":
                block = array.shape[0] // 4
                pairs = [(part_rows(src, at.mate * block, block), dst.at[0]), (part_rows(src, at.far_mate * block, block), dst.at[1])]
            for s, d in pairs:
                n = len(made)
                made.append(pltpu.make_async_remote_copy(s, d, send.at[n], recv.at[n], device_id=at.to["mate" if to == "term" else to], device_id_type=MESH))
        return made


IDS = {"gate_up": 0, "down": 1}


def hosted(kernel, grid, flops, operands, in_specs, out_specs, out_shape, scratch, sends, after, name, aliases=None):
    ins, outs, count = len(operands), len(out_shape), len(sends.items)
    collective = IDS.setdefault(name, len(IDS)) if count else None

    def body(*refs):
        own_in, sources, rest = refs[:ins], refs[ins : ins + count], refs[ins + count + 1 :]
        own_out, targets, rest = rest[:outs], rest[outs : outs + count], rest[outs + count :]
        own_scratch, sems = rest[: len(scratch)], rest[len(scratch) :]
        step = pl.program_id(0)
        if count:

            @pl.when(step == 0)
            def _():
                at = Place()
                at.greet(sends.whom)
                for copy in sends.copies(at, sources, targets, *sems):
                    copy.start()

        kernel(*own_in, *own_out, *own_scratch)
        if count:

            @pl.when(step == grid - 1)
            def _():
                for copy in sends.copies(Place(), sources, targets, *sems):
                    copy.wait()

    results = pl.pallas_call(
        body,
        grid=(grid,),
        cost_estimate=cost(flops),
        compiler_params=params(collective),
        in_specs=list(in_specs) + [ANY] * (count + 1),
        out_specs=list(out_specs) + [ANY] * count,
        out_shape=list(out_shape) + sends.out_shape,
        scratch_shapes=list(scratch) + sends.scratch,
        input_output_aliases=aliases or {},
        name=name,
    )(*operands, *sends.arrays, after)
    return results[:outs], results[outs:]


def first_kernel(x, weights):
    tokens, d = x.shape
    ff = weights["g"].shape[2]
    width, tile = ff // CHUNKS, min(512, tokens)
    tiles = tokens // tile
    part = min(256, width)
    units = []
    for c in range(CHUNKS):
        units += [Unit("g", 0, c * width, width), Unit("u", 0, c * width, width)]
    groups = [(2 * c, 2 * c + 1) for c in range(CHUNKS)]
    for name, layer, which in (("d", 0, (0, 1)), ("g", 1, (0, 1)), ("u", 1, (0,))):
        columns = weights[name].shape[2] // 2
        for n in which:
            groups.append((len(units),))
            units.append(Unit(name, layer, n * columns, columns))
    names = list(weights)
    total_steps = CHUNKS * tiles
    def step_of(time):
        return max(0, int((time - 29.0) / 2.55) + 1)

    events = {}
    for k in range(len(groups)):
        if k >= 2:
            events.setdefault(min(step_of(11.0 * (k + 1) + 3), total_steps - 1), []).append(("x", k))
        if k >= 1:
            events.setdefault(min(step_of(11.0 * (k + 2) + 6), total_steps - 1), []).append(("y", k))

    def kernel(x_ref, *refs):
        w_refs = dict(zip(names, refs[:3], strict=True))
        s_ref, q_ref, h_ref, a_ref = refs[3:7]
        buffers = refs[7 : 7 + len(units)]
        normal, wg, wu, load_sems, send, recv = refs[7 + len(units) :]
        step = pl.program_id(0)
        chunk, row = step // tiles, step % tiles
        move = Mover(units, w_refs, buffers, send, recv)

        def over_x(k):
            move.arrived(groups[k], "x")
            move.start(groups[k], "y", "straight")
            if k + 2 < len(groups):
                move.start(groups[k + 2], "x")

        def over_y(k):
            move.arrived(groups[k], "y")
            move.start(groups[k], "around")

        @pl.when(step == 0)
        def _():
            move.at.greet(("mate", "x", "y"))
            move.start(groups[0], "x")
            move.start(groups[1], "x")
            for group in groups:
                move.start(group, "own")

        @pl.when(chunk == 0)
        def _():
            a_ref[...] = normal[pl.ds(pl.multiple_of(row * tile, tile), tile)] = normed(x_ref[...].astype(F32)).astype(BF16)

        @pl.when(step == 0)
        def _():
            over_x(0)
            over_x(1)
            over_y(0)

        for at, these in events.items():

            @pl.when(step == at)
            def _():
                for kind, k in these:
                    (over_x if kind == "x" else over_y)(k)

        for c in range(CHUNKS):

            @pl.when(step == c * tiles)
            def _():
                move.arrived(groups[c], "own", "straight", "around")
                pairs = [([(units[n], w_refs[units[n].name], buffers[n])], scratch) for n, scratch in zip(groups[c], (wg, wu), strict=True)]
                for copy in load(pairs, load_sems):
                    copy.wait()

        av = normal[pl.ds(pl.multiple_of(row * tile, tile), tile)]
        for j in range(0, width, part):
            at = pl.ds(j, part)
            g, u = dot(av, wg[:, at]), dot(av, wu[:, at])
            s = sigmoid(g)
            sl = g * s
            s_ref[:, at] = sl
            q_ref[:, at] = u * (s + sl * (1.0 - s))
            h_ref[:, at] = (sl * u).astype(BF16)

        @pl.when(step == total_steps - 1)
        def _():
            for k in range(CHUNKS, len(groups)):
                move.arrived(groups[k], "own", "straight", "around")
            move.sent(range(len(units)))

    once = pl.BlockSpec((tile, d), lambda i: (jnp.minimum(i, tiles - 1), 0))
    out = pl.BlockSpec((tile, width), lambda i: (i % tiles, i // tiles))
    results = pl.pallas_call(
        kernel,
        grid=(total_steps,),
        cost_estimate=cost(4 * tokens * d * ff),
        compiler_params=params(0),
        in_specs=[once] + [ANY] * 3,
        out_specs=[out] * 3 + [once] + [ANY] * len(units),
        out_shape=[shaped(tokens, ff, dtype=F32)] * 2
        + [shaped(tokens, ff), shaped(tokens, d)]
        + [shaped(4 * weights[unit.name].shape[1], unit.width) for unit in units],
        scratch_shapes=[pltpu.VMEM((tokens, d), BF16)]
        + [pltpu.VMEM((d, width), BF16)] * 2
        + [pltpu.SemaphoreType.DMA((8,)), pltpu.SemaphoreType.DMA((len(units), 5)), pltpu.SemaphoreType.DMA((len(units), 5))],
        name="gate_up",
    )(x, *weights.values())
    kept, buffers = results[:4], results[4:]
    gathered = {}
    for unit, buf in zip(units, buffers, strict=True):
        gathered.setdefault((unit.name, unit.layer), []).append((unit, buf))
    return kept, gathered


def second_kernel(hidden, h, w, weights):
    tokens, ff = hidden.shape
    d = h.shape[1]
    tile = min(256, tokens)
    steps = tokens // tile
    half_u, half_d = weights["u"].shape[2] // 2, weights["d"].shape[2] // 2
    units = [Unit("u", 1, half_u, half_u), Unit("d", 1, 0, half_d), Unit("d", 1, half_d, half_d)]
    names = ("u", "d")
    events = {5: [("x", 0)], 9: [("x", 1)], 10: [("y", 0)], 13: [("x", 2)], 14: [("y", 1)], 15: [("y", 2)]}
    events = {min(at, steps - 1): these for at, these in events.items()} if steps >= 16 else {steps - 1: [(kind, k) for k in range(3) for kind in "xy"]}
    count = len(w.operands)

    def kernel(hidden_ref, h_ref, *refs):
        ins, refs = refs[:count], refs[count:]
        w_refs = dict(zip(names, refs[:2], strict=True))
        o_ref, a_ref = refs[2:4]
        buffers = refs[4:7]
        wd, load_sems, send, recv = refs[7:]
        step = pl.program_id(0)
        move = Mover(units, w_refs, buffers, send, recv)

        @pl.when(step == 0)
        def _():
            move.at.greet(("mate", "x", "y"))
            move.start((0, 1), "x")
            move.start(range(3), "own")

        fetch((w,), ins, (wd,), load_sems)
        out = (h_ref[...].astype(F32) + rounded(dot(hidden_ref[...], wd[...]))).astype(BF16)
        o_ref[...] = out
        a_ref[...] = normed(out.astype(F32)).astype(BF16)

        for at, these in events.items():

            @pl.when(step == at)
            def _():
                for kind, k in these:
                    if kind == "x":
                        move.arrived((k,), "x")
                        move.start((k,), "y", "straight")
                        if k == 0:
                            move.start((2,), "x")
                    else:
                        move.arrived((k,), "y")
                        move.start((k,), "around")

        @pl.when(step == steps - 1)
        def _():
            move.arrived(range(3), "own", "straight", "around")
            move.sent(range(3))

    results = pl.pallas_call(
        kernel,
        grid=(steps,),
        cost_estimate=cost(2 * tokens * d * ff),
        compiler_params=params(1),
        in_specs=[rows(tile, ff), rows(tile, d)] + [ANY] * (count + 2),
        out_specs=[rows(tile, d)] * 2 + [ANY] * 3,
        out_shape=[shaped(tokens, d)] * 2 + [shaped(4 * weights[unit.name].shape[1], unit.width) for unit in units],
        scratch_shapes=[
            pltpu.VMEM((ff, d), BF16),
            pltpu.SemaphoreType.DMA((w.copies,)),
            pltpu.SemaphoreType.DMA((3, 5)),
            pltpu.SemaphoreType.DMA((3, 5)),
        ],
        name="down",
    )(hidden, h, *w.operands, weights["u"], weights["d"])
    return results[:2], list(zip(units, results[2:], strict=True))


def scratch_for(*matrices):
    return [pltpu.VMEM(m.shape, BF16) for m in matrices] + [pltpu.SemaphoreType.DMA((sum(m.copies for m in matrices),))]


def operands_of(*matrices):
    return [operand for m in matrices for operand in m.operands]


def last_layer(a, dy, gate, up, w):
    tokens, d = a.shape
    ff = gate.shape[1]
    tile, part = min(256, tokens), 256
    matrices = (gate, up, w)
    weights = operands_of(*matrices)

    def kernel(a_ref, dy_ref, *refs):
        ins, (h_ref, dg_ref, du_ref, wg, wu, wd, sems) = refs[: len(weights)], refs[len(weights) :]
        fetch(matrices, ins, (wg, wu, wd), sems)
        av, dyv = a_ref[...], dy_ref[...]
        for j in range(0, ff, part):
            at = pl.ds(j, part)
            g, u, dh = dot(av, wg[:, at]), dot(av, wu[:, at]), rounded(dot_nt(dyv, wd[at, :]))
            s = sigmoid(g)
            sl = g * s
            h_ref[:, at] = (sl * u).astype(BF16)
            dg_ref[:, at] = (dh * (u * (s + sl * (1.0 - s)))).astype(BF16)
            du_ref[:, at] = (dh * sl).astype(BF16)

    return hosted(
        kernel,
        tokens // tile,
        6 * tokens * d * ff,
        [a, dy, *weights],
        [rows(tile, d)] * 2 + [ANY] * len(weights),
        [rows(tile, ff)] * 3,
        [shaped(tokens, ff)] * 3,
        scratch_for(*matrices),
        Sends(),
        a,
        "last_layer",
    )[0]


def hidden_back(dy, silu, slope, w, sends, after):
    tokens, d = dy.shape
    ff = silu.shape[1]
    tile, part = min(256, tokens), 256
    weights = w.operands

    def kernel(dy_ref, s_ref, q_ref, *refs):
        ins, (dg_ref, du_ref, wd, sems) = refs[: len(weights)], refs[len(weights) :]
        fetch((w,), ins, (wd,), sems)
        dyv = dy_ref[...]
        for j in range(0, ff, part):
            at = pl.ds(j, part)
            dh = rounded(dot_nt(dyv, wd[at, :]))
            dg_ref[:, at] = (dh * q_ref[:, at]).astype(BF16)
            du_ref[:, at] = (dh * s_ref[:, at]).astype(BF16)

    return hosted(
        kernel,
        tokens // tile,
        2 * tokens * d * ff,
        [dy, silu, slope, *weights],
        [rows(tile, d)] + [rows(tile, ff)] * 2 + [ANY] * len(weights),
        [rows(tile, ff)] * 2,
        [shaped(tokens, ff)] * 2,
        scratch_for(w),
        sends,
        after,
        "hidden_back",
    )


def norm_back(da, wide, dres):
    scale = lax.rsqrt(jnp.mean(wide * wide, -1, keepdims=True) + 1e-6)
    along = jnp.sum(da * wide, -1, keepdims=True) * (scale * scale * scale) * (1.0 / wide.shape[-1])
    return (dres + rounded(da * scale - wide * along)).astype(BF16)


def input_back(dg, du, h, dres, gate, up, sends, after):
    tokens, ff = dg.shape
    d = h.shape[1]
    tile = min(256, tokens)
    weights = operands_of(gate, up)

    def kernel(dg_ref, du_ref, h_ref, r_ref, *refs):
        ins, (o_ref, wg, wu, sems) = refs[: len(weights)], refs[len(weights) :]
        fetch((gate, up), ins, (wg, wu), sems)
        da = rounded(rounded(dot_nt(dg_ref[...], wg[...])) + rounded(dot_nt(du_ref[...], wu[...])))
        o_ref[...] = norm_back(da, h_ref[...].astype(F32), r_ref[...].astype(F32))

    return hosted(
        kernel,
        tokens // tile,
        4 * tokens * d * ff,
        [dg, du, h, dres, *weights],
        [rows(tile, ff)] * 2 + [rows(tile, d)] * 2 + [ANY] * len(weights),
        [rows(tile, d)],
        [shaped(tokens, d)],
        scratch_for(gate, up),
        sends,
        after,
        "input_back",
    )


def input_back_gate(dg, gate, part, parts, sends, after):
    tokens, ff = dg.shape[0] // parts, dg.shape[1]
    d = gate.shape[0]
    tile = min(256, tokens)
    first = part * (tokens // tile)
    weights = gate.operands

    def kernel(dg_ref, *refs):
        ins, (o_ref, wg, sems) = refs[: len(weights)], refs[len(weights) :]
        fetch((gate,), ins, (wg,), sems)
        o_ref[...] = dot_nt(dg_ref[...], wg[...]).astype(BF16)

    return hosted(
        kernel,
        tokens // tile,
        2 * tokens * d * ff,
        [dg, *weights],
        [pl.BlockSpec((tile, ff), lambda i: (i + first, 0))] + [ANY] * len(weights),
        [rows(tile, d)],
        [shaped(tokens, d)],
        scratch_for(gate),
        sends,
        after,
        f"input_back_gate_{part}",
    )


def input_back_up(du, from_gate, h, dres, up, sends, after):
    tokens, ff = du.shape
    d = h.shape[1]
    tile = min(256, tokens)
    split = (tokens // tile) // 2
    weights = up.operands

    def kernel(du_ref, f0_ref, f1_ref, h_ref, r_ref, *refs):
        ins, (o_ref, wu, sems) = refs[: len(weights)], refs[len(weights) :]
        fetch((up,), ins, (wu,), sems)
        first = jnp.where(pl.program_id(0) < split, f0_ref[...].astype(F32), f1_ref[...].astype(F32))
        da = rounded(first + rounded(dot_nt(du_ref[...], wu[...])))
        o_ref[...] = norm_back(da, h_ref[...].astype(F32), r_ref[...].astype(F32))

    return hosted(
        kernel,
        tokens // tile,
        2 * tokens * d * ff,
        [du, *from_gate, h, dres, *weights],
        [
            rows(tile, ff),
            pl.BlockSpec((tile, d), lambda i: (jnp.minimum(i, split - 1), 0)),
            pl.BlockSpec((tile, d), lambda i: (jnp.maximum(i - split, 0), 0)),
            rows(tile, d),
            rows(tile, d),
        ]
        + [ANY] * len(weights),
        [rows(tile, d)],
        [shaped(tokens, d)],
        scratch_for(up),
        sends,
        after,
        "input_back_up",
    )


def whole_block(shape):
    return pl.BlockSpec(shape, lambda i: (0, 0), pipeline_mode=pl.Buffered(1))


def grad_in(a, b, sends, after, name, part=0, parts=1):
    tokens, d = a.shape
    width = b.shape[1] // parts
    tile = min(512, width)
    first = part * (width // tile)

    def kernel(a_ref, b_ref, o_ref):
        o_ref[...] = dot_tn(a_ref[...], b_ref[...]).astype(BF16)

    (term,), arrived = hosted(
        kernel,
        width // tile,
        2 * tokens * d * width,
        [a, b],
        [whole_block((tokens, d)), pl.BlockSpec((tokens, tile), lambda i: (0, i + first))],
        [pl.BlockSpec((d, tile), lambda i: (0, i))],
        [shaped(d, width)],
        [],
        sends,
        after,
        name,
    )
    return term, arrived


def grad_out(hidden, dy, sends, after, name):
    tokens, d = dy.shape
    ff = hidden.shape[1]
    tile = min(512, ff)

    def kernel(hidden_ref, dy_ref, o_ref):
        o_ref[...] = dot_tn(hidden_ref[...], dy_ref[...]).astype(BF16)

    (term,), arrived = hosted(
        kernel,
        ff // tile,
        2 * tokens * d * ff,
        [hidden, dy],
        [pl.BlockSpec((tokens, tile), lambda i: (0, i)), whole_block((tokens, d))],
        [rows(tile, d)],
        [shaped(ff, d)],
        [],
        sends,
        after,
        name,
    )
    return term, arrived


def total(*terms):
    return sum(t.astype(F32) for t in terms).astype(BF16)


def solution(mesh):
    def block_of(term, which):
        size = term.shape[0] // 4
        return lax.dynamic_slice_in_dim(term, which * size, size, 0)

    def step(x, dy, w_gate, w_up, w_down):
        x, dy = x[0], dy[0]
        weights = {"g": w_gate, "u": w_up, "d": w_down}
        me = lax.axis_index("s")
        far = (me + 2) % 4

        (silu, slope, hidden0, a0), gathered = first_kernel(x, weights)

        def whole(name, layer):
            units, buffers = zip(*gathered[name, layer], strict=True)
            return Whole(weights[name], units, buffers)

        gate0, up0, down0 = (whole(name, 0) for name in "gud")
        (h1, a1), rest = second_kernel(hidden0, x, down0, weights)
        for unit, buf in rest:
            gathered.setdefault((unit.name, unit.layer), []).append((unit, buf))
        gate1, up1, down1 = (whole(name, 1) for name in "gud")
        hidden1, dg1, du1 = last_layer(a1, dy, gate1, up1, down1)

        def for_x(term, received):
            return total(block_of(term, far), received[1])

        def for_y(term, received, over_x):
            return total(block_of(term, me), received[0], over_x)

        wd1, _ = grad_out(hidden1, dy, Sends(), dy, "wd1")
        wg1, (r_wd1,) = grad_in(a1, dg1, Sends((wd1, "term")), dy, "wg1")
        wu1, (x_wd1, r_wg1) = grad_in(a1, du1, Sends((for_x(wd1, r_wd1), "x"), (wg1, "term")), dy, "wu1")
        s_wd1 = for_y(wd1, r_wd1, x_wd1)
        (dh,), (y_wd1, x_wg1, r_wu1) = input_back(dg1, du1, h1, dy, gate1, up1, Sends((s_wd1, "y"), (for_x(wg1, r_wg1), "x"), (wu1, "term")), dy)
        s_wg1 = for_y(wg1, r_wg1, x_wg1)
        wd0, (y_wg1, x_wu1) = grad_out(hidden0, dh, Sends((s_wg1, "y"), (for_x(wu1, r_wu1), "x")), dh, "wd0")
        s_wu1 = for_y(wu1, r_wu1, x_wu1)
        (dg0, du0), (y_wu1, r_wd0) = hidden_back(dh, silu, slope, down0, Sends((s_wu1, "y"), (wd0, "term")), dh)
        wg0, (x_wd0,) = grad_in(a0, dg0, Sends((for_x(wd0, r_wd0), "x")), dh, "wg0")
        s_wd0 = for_y(wd0, r_wd0, x_wd0)
        wu0, (y_wd0, r_wg0) = grad_in(a0, du0, Sends((s_wd0, "y"), (wg0, "term")), dh, "wu0")
        (b0,), (x_wg0, r_wu0) = input_back_gate(dg0, gate0, 0, 2, Sends((for_x(wg0, r_wg0), "x"), (wu0, "term")), dh)
        s_wg0 = for_y(wg0, r_wg0, x_wg0)
        (b1,), (y_wg0, x_wu0) = input_back_gate(dg0, gate0, 1, 2, Sends((s_wg0, "y"), (for_x(wu0, r_wu0), "x")), b0)
        s_wu0 = for_y(wu0, r_wu0, x_wu0)
        (dx,), (y_wu0,) = input_back_up(du0, (b0, b1), x, dh, up0, Sends((s_wu0, "y")), b1)

        return (
            dx[None],
            jnp.stack([total(s_wg0, y_wg0), total(s_wg1, y_wg1)]),
            jnp.stack([total(s_wu0, y_wu0), total(s_wu1, y_wu1)]),
            jnp.stack([total(s_wd0, y_wd0), total(s_wd1, y_wd1)]),
        )

    states, cut = P(("rep", "r", "s"), None, None), P(None, "s", None)
    return jax.shard_map(
        step,
        mesh=mesh,
        in_specs=(states, states) + (cut,) * 3,
        out_specs=(states,) + (P("rep", "s", None),) * 3,
        check_vma=False,
    )
```

```python
import jax
import jax.numpy as jnp
from jax import lax
from jax.experimental import pallas as pl
from jax.experimental.pallas import tpu as pltpu
from jax.sharding import PartitionSpec as P

F32, BF16 = jnp.float32, jnp.bfloat16
ANY = pl.BlockSpec(memory_space=pl.ANY)
MESH = pl.DeviceIdType.MESH
NT = (((1,), (1,)), ((), ()))
TN = (((0,), (0,)), ((), ()))
CHUNKS = 4


def dot(a, b):
    return jnp.dot(a, b, preferred_element_type=F32)


def dot_nt(a, b):
    return lax.dot_general(a, b, NT, preferred_element_type=F32)


def dot_tn(a, b):
    return lax.dot_general(a, b, TN, preferred_element_type=F32)


def rounded(v):
    return v.astype(BF16).astype(F32)


def sigmoid(g):
    return pl.reciprocal(1.0 + jnp.exp(-g))


def normed(wide):
    return wide * lax.rsqrt(jnp.mean(wide * wide, -1, keepdims=True) + 1e-6)


def rows(tile, width):
    return pl.BlockSpec((tile, width), lambda i: (i, 0))


def shaped(*shape, dtype=BF16):
    return jax.ShapeDtypeStruct(shape, dtype)


class Place:
    def __init__(self):
        self.me, self.y = lax.axis_index("s"), lax.axis_index("r")
        x, c = self.me // 2, self.me % 2
        self.mate, self.far, self.far_mate = 2 * x + 1 - c, 2 * (1 - x) + c, 2 * (1 - x) + 1 - c
        self.to = {"mate": {"s": self.mate}, "x": {"s": self.far}, "y": {"r": 1 - self.y}}

    def greet(self, whom):
        barrier = pltpu.get_barrier_semaphore()
        for name in whom:
            pl.semaphore_signal(barrier, inc=1, device_id=self.to[name], device_id_type=MESH)
        pl.semaphore_wait(barrier, len(whom))


def part_rows(ref, start, size):
    return ref.at[pl.ds(pl.multiple_of(start, 16), size)]


def params(collective=None):
    more = {} if collective is None else dict(collective_id=collective, has_side_effects=True)
    return pltpu.CompilerParams(dimension_semantics=("arbitrary",), vmem_limit_bytes=62 << 20, **more)


def cost(flops):
    return pl.CostEstimate(flops=flops, bytes_accessed=1 << 20, transcendentals=0)


class Unit:
    def __init__(self, name, layer, start, width):
        self.name, self.layer, self.start, self.width = name, layer, start, width


class Mover:
    KINDS = ("own", "x", "y", "straight", "around")

    def __init__(self, units, weights, buffers, send, recv):
        self.units, self.weights, self.buffers, self.send, self.recv = units, weights, buffers, send, recv
        self.at = Place()

    def copy(self, n, kind, arriving=False):
        unit, buf, at = self.units[n], self.buffers[n], self.at
        block = buf.shape[0] // 4
        half = block // 2
        w = self.weights[unit.name].at[unit.layer]
        cols = pl.ds(unit.start, unit.width)
        mine, other = at.y * half, (1 - at.y) * half
        if arriving:
            start, size = {
                "own": (at.mate * block, block),
                "x": (at.far * block + mine, half),
                "y": (at.far * block + other, half),
                "straight": (at.far_mate * block + mine, half),
                "around": (at.far_mate * block + other, half),
            }[kind]
            src = dst = part_rows(buf, start, size)
        elif kind == "own":
            src, dst = w.at[:, cols], part_rows(buf, at.me * block, block)
        elif kind == "x":
            src, dst = w.at[pl.ds(pl.multiple_of(mine, 16), half), cols], part_rows(buf, at.me * block + mine, half)
        else:
            src = dst = part_rows(buf, at.far * block + (other if kind == "around" else mine), half)
        k = self.KINDS.index(kind)
        to = at.to[{"x": "x", "y": "y"}.get(kind, "mate")]
        return pltpu.make_async_remote_copy(src, dst, self.send.at[n, k], self.recv.at[n, k], device_id=to, device_id_type=MESH)

    def start(self, ns, *kinds):
        for n in ns:
            for kind in kinds:
                self.copy(n, kind).start()

    def arrived(self, ns, *kinds):
        for n in ns:
            for kind in kinds:
                self.copy(n, kind, arriving=True).wait_recv()

    def sent(self, ns):
        for n in ns:
            for kind in self.KINDS:
                self.copy(n, kind).wait_send()


def load(pairs, sems, first=0):
    at, made = Place(), []
    for units, scratch in pairs:
        col = 0
        for unit, w, buf in units:
            block = buf.shape[0] // 4
            for n, who in enumerate((at.me, at.mate, at.far, at.far_mate)):
                src = w.at[unit.layer, :, pl.ds(unit.start, unit.width)] if n == 0 else part_rows(buf, who * block, block)
                dst = scratch.at[pl.ds(pl.multiple_of(who * block, 16), block), pl.ds(col, unit.width)]
                made.append(pltpu.make_async_copy(src, dst, sems.at[first + len(made)]))
                made[-1].start()
            col += unit.width
    return made


class Whole:
    def __init__(self, w, units, buffers):
        self.w, self.units, self.buffers = w, units, buffers
        self.operands = [w, *buffers]
        self.shape = (4 * w.shape[1], w.shape[2])
        self.copies = 4 * len(units)

    def pairs(self, refs):
        return [(unit, refs[0], buf) for unit, buf in zip(self.units, refs[1:], strict=True)]


def fetch(matrices, refs, scratches, sems):
    @pl.when(pl.program_id(0) == 0)
    def _():
        pairs, used = [], 0
        for matrix, scratch in zip(matrices, scratches, strict=True):
            count = len(matrix.operands)
            pairs.append((matrix.pairs(refs[used : used + count]), scratch))
            used += count
        for copy in load(pairs, sems):
            copy.wait()


def first_kernel(x, weights):
    tokens, d = x.shape
    ff = weights["g"].shape[2]
    width, tile = ff // CHUNKS, min(512, tokens)
    tiles = tokens // tile
    part = min(256, width)
    units = []
    for c in range(CHUNKS):
        units += [Unit("g", 0, c * width, width), Unit("u", 0, c * width, width)]
    groups = [(2 * c, 2 * c + 1) for c in range(CHUNKS)]
    for name, layer, which in (("d", 0, (0, 1)), ("g", 1, (0, 1)), ("u", 1, (0,))):
        columns = weights[name].shape[2] // 2
        for n in which:
            groups.append((len(units),))
            units.append(Unit(name, layer, n * columns, columns))
    names = list(weights)
    total_steps = CHUNKS * tiles
    def step_of(time):
        return max(0, int((time - 29.0) / 2.55) + 1)

    events = {}
    for k in range(len(groups)):
        if k >= 2:
            events.setdefault(min(step_of(11.0 * (k + 1) + 3), total_steps - 1), []).append(("x", k))
        if k >= 1:
            events.setdefault(min(step_of(11.0 * (k + 2) + 6), total_steps - 1), []).append(("y", k))

    def kernel(x_ref, *refs):
        w_refs = dict(zip(names, refs[:3], strict=True))
        s_ref, q_ref, h_ref, a_ref = refs[3:7]
        buffers = refs[7 : 7 + len(units)]
        normal, wg, wu, load_sems, send, recv = refs[7 + len(units) :]
        step = pl.program_id(0)
        chunk, row = step // tiles, step % tiles
        move = Mover(units, w_refs, buffers, send, recv)

        def over_x(k):
            move.arrived(groups[k], "x")
            move.start(groups[k], "y", "straight")
            if k + 2 < len(groups):
                move.start(groups[k + 2], "x")

        def over_y(k):
            move.arrived(groups[k], "y")
            move.start(groups[k], "around")

        @pl.when(step == 0)
        def _():
            move.at.greet(("mate", "x", "y"))
            move.start(groups[0], "x")
            move.start(groups[1], "x")
            for group in groups:
                move.start(group, "own")

        @pl.when(chunk == 0)
        def _():
            a_ref[...] = normal[pl.ds(pl.multiple_of(row * tile, tile), tile)] = normed(x_ref[...].astype(F32)).astype(BF16)

        @pl.when(step == 0)
        def _():
            over_x(0)
            over_x(1)
            over_y(0)

        for at, these in events.items():

            @pl.when(step == at)
            def _():
                for kind, k in these:
                    (over_x if kind == "x" else over_y)(k)

        for c in range(CHUNKS):

            @pl.when(step == c * tiles)
            def _():
                move.arrived(groups[c], "own", "straight", "around")
                pairs = [([(units[n], w_refs[units[n].name], buffers[n])], scratch) for n, scratch in zip(groups[c], (wg, wu), strict=True)]
                for copy in load(pairs, load_sems):
                    copy.wait()

        av = normal[pl.ds(pl.multiple_of(row * tile, tile), tile)]
        for j in range(0, width, part):
            at = pl.ds(j, part)
            g, u = dot(av, wg[:, at]), dot(av, wu[:, at])
            s = sigmoid(g)
            sl = g * s
            s_ref[:, at] = sl
            q_ref[:, at] = u * (s + sl * (1.0 - s))
            h_ref[:, at] = (sl * u).astype(BF16)

        @pl.when(step == total_steps - 1)
        def _():
            for k in range(CHUNKS, len(groups)):
                move.arrived(groups[k], "own", "straight", "around")
            move.sent(range(len(units)))

    once = pl.BlockSpec((tile, d), lambda i: (jnp.minimum(i, tiles - 1), 0))
    out = pl.BlockSpec((tile, width), lambda i: (i % tiles, i // tiles))
    results = pl.pallas_call(
        kernel,
        grid=(total_steps,),
        cost_estimate=cost(4 * tokens * d * ff),
        compiler_params=params(0),
        in_specs=[once] + [ANY] * 3,
        out_specs=[out] * 3 + [once] + [ANY] * len(units),
        out_shape=[shaped(tokens, ff, dtype=F32)] * 2
        + [shaped(tokens, ff), shaped(tokens, d)]
        + [shaped(4 * weights[unit.name].shape[1], unit.width) for unit in units],
        scratch_shapes=[pltpu.VMEM((tokens, d), BF16)]
        + [pltpu.VMEM((d, width), BF16)] * 2
        + [pltpu.SemaphoreType.DMA((8,)), pltpu.SemaphoreType.DMA((len(units), 5)), pltpu.SemaphoreType.DMA((len(units), 5))],
        name="gate_up",
    )(x, *weights.values())
    kept, buffers = results[:4], results[4:]
    gathered = {}
    for unit, buf in zip(units, buffers, strict=True):
        gathered.setdefault((unit.name, unit.layer), []).append((unit, buf))
    return kept, gathered


def second_kernel(hidden, h, w, weights):
    tokens, ff = hidden.shape
    d = h.shape[1]
    tile = min(256, tokens)
    steps = tokens // tile
    half_u, half_d = weights["u"].shape[2] // 2, weights["d"].shape[2] // 2
    units = [Unit("u", 1, half_u, half_u), Unit("d", 1, 0, half_d), Unit("d", 1, half_d, half_d)]
    names = ("u", "d")
    events = {5: [("x", 0)], 9: [("x", 1)], 10: [("y", 0)], 13: [("x", 2)], 14: [("y", 1)], 15: [("y", 2)]}
    events = {min(at, steps - 1): these for at, these in events.items()} if steps >= 16 else {steps - 1: [(kind, k) for k in range(3) for kind in "xy"]}
    count = len(w.operands)

    def kernel(hidden_ref, h_ref, *refs):
        ins, refs = refs[:count], refs[count:]
        w_refs = dict(zip(names, refs[:2], strict=True))
        o_ref, a_ref = refs[2:4]
        buffers = refs[4:7]
        wd, load_sems, send, recv = refs[7:]
        step = pl.program_id(0)
        move = Mover(units, w_refs, buffers, send, recv)

        @pl.when(step == 0)
        def _():
            move.at.greet(("mate", "x", "y"))
            move.start((0, 1), "x")
            move.start(range(3), "own")

        fetch((w,), ins, (wd,), load_sems)
        out = (h_ref[...].astype(F32) + rounded(dot(hidden_ref[...], wd[...]))).astype(BF16)
        o_ref[...] = out
        a_ref[...] = normed(out.astype(F32)).astype(BF16)

        for at, these in events.items():

            @pl.when(step == at)
            def _():
                for kind, k in these:
                    if kind == "x":
                        move.arrived((k,), "x")
                        move.start((k,), "y", "straight")
                        if k == 0:
                            move.start((2,), "x")
                    else:
                        move.arrived((k,), "y")
                        move.start((k,), "around")

        @pl.when(step == steps - 1)
        def _():
            move.arrived(range(3), "own", "straight", "around")
            move.sent(range(3))

    results = pl.pallas_call(
        kernel,
        grid=(steps,),
        cost_estimate=cost(2 * tokens * d * ff),
        compiler_params=params(1),
        in_specs=[rows(tile, ff), rows(tile, d)] + [ANY] * (count + 2),
        out_specs=[rows(tile, d)] * 2 + [ANY] * 3,
        out_shape=[shaped(tokens, d)] * 2 + [shaped(4 * weights[unit.name].shape[1], unit.width) for unit in units],
        scratch_shapes=[
            pltpu.VMEM((ff, d), BF16),
            pltpu.SemaphoreType.DMA((w.copies,)),
            pltpu.SemaphoreType.DMA((3, 5)),
            pltpu.SemaphoreType.DMA((3, 5)),
        ],
        name="down",
    )(hidden, h, *w.operands, weights["u"], weights["d"])
    return results[:2], list(zip(units, results[2:], strict=True))


def scratch_for(*matrices):
    return [pltpu.VMEM(m.shape, BF16) for m in matrices] + [pltpu.SemaphoreType.DMA((sum(m.copies for m in matrices),))]


def operands_of(*matrices):
    return [operand for m in matrices for operand in m.operands]


def last_layer(a, dy, gate, up, w):
    tokens, d = a.shape
    ff = gate.shape[1]
    tile, part = min(256, tokens), 256
    matrices = (gate, up, w)
    weights = operands_of(*matrices)

    def kernel(a_ref, dy_ref, *refs):
        ins, (h_ref, dg_ref, du_ref, wg, wu, wd, sems) = refs[: len(weights)], refs[len(weights) :]
        fetch(matrices, ins, (wg, wu, wd), sems)
        av, dyv = a_ref[...], dy_ref[...]
        for j in range(0, ff, part):
            at = pl.ds(j, part)
            g, u, dh = dot(av, wg[:, at]), dot(av, wu[:, at]), rounded(dot_nt(dyv, wd[at, :]))
            s = sigmoid(g)
            sl = g * s
            h_ref[:, at] = (sl * u).astype(BF16)
            dg_ref[:, at] = (dh * (u * (s + sl * (1.0 - s)))).astype(BF16)
            du_ref[:, at] = (dh * sl).astype(BF16)

    return pl.pallas_call(
        kernel,
        grid=(tokens // tile,),
        cost_estimate=cost(6 * tokens * d * ff),
        compiler_params=params(),
        in_specs=[rows(tile, d)] * 2 + [ANY] * len(weights),
        out_specs=[rows(tile, ff)] * 3,
        out_shape=[shaped(tokens, ff)] * 3,
        scratch_shapes=scratch_for(*matrices),
        name="last_layer",
    )(a, dy, *weights)


def norm_back(da, wide, dres):
    scale = lax.rsqrt(jnp.mean(wide * wide, -1, keepdims=True) + 1e-6)
    along = jnp.sum(da * wide, -1, keepdims=True) * (scale * scale * scale) * (1.0 / wide.shape[-1])
    return (dres + rounded(da * scale - wide * along)).astype(BF16)


class Part:
    def __init__(self, name, term_shape, start, width):
        self.name, self.start, self.width = name, start, width
        self.block = term_shape[0] // 4

    def arrays(self):
        one = shaped(self.block, self.width)
        return {"r": shaped(2, self.block, self.width), "s": one, "x": one, "b": one, "y": one}


def backward(x, dy, a0, a1, h1, hidden0, hidden1, silu, slope, dg1, du1, gate0, up0, down0, gate1, up1):
    tokens, d = x.shape
    ff = silu.shape[1]
    shapes = {"wg": (d, ff), "wu": (d, ff), "wd": (ff, d)}
    terms = {name + layer: shaped(*shapes[name]) for layer in "10" for name in ("wd", "wg", "wu")}
    parts = [Part(name, terms[name].shape, 0, terms[name].shape[1]) for name in ("wd1", "wg1", "wu1", "wd0", "wg0")]
    parts += [Part("wu0", shapes["wu"], n * (ff // 2), ff // 2) for n in range(2)]
    WD1, WG1, WU1, WD0, WG0, WU0, WU0B = range(7)
    matrices = {"gate0": gate0, "up0": up0, "down0": down0, "gate1": gate1, "up1": up1}
    plain = {"x": x, "dy": dy, "a0": a0, "a1": a1, "h1": h1, "hidden0": hidden0, "hidden1": hidden1, "silu": silu, "slope": slope, "dg1": dg1, "du1": du1}
    operands = list(plain.values()) + operands_of(*matrices.values())
    made = {"dx": shaped(tokens, d), "dh": shaped(tokens, d), "dg0": shaped(tokens, ff), "du0": shaped(tokens, ff), **terms}
    part_arrays = [part.arrays() for part in parts]
    out_shape = list(made.values()) + [one for group in part_arrays for one in group.values()]
    tile = min(256, tokens)
    col = min(512, ff)

    def kernel(*refs):
        refs = list(refs)

        def take(n):
            taken, refs[:] = refs[:n], refs[n:]
            return taken

        ref = dict(zip(plain, take(len(plain)), strict=True))
        weight = {name: take(len(m.operands)) for name, m in matrices.items()}
        ref.update(zip(made, take(len(made)), strict=True))
        bufs = [dict(zip(group, take(len(group)), strict=True)) for group in part_arrays]
        send, recv, load_sems, add_sems = refs
        at = Place()

        def transfer(n, kind):
            part, buf = parts[n], bufs[n]
            base = 4 * n
            if kind == "mate":
                cols = pl.ds(part.start, part.width)
                pairs = [(part_rows(ref[part.name], who * part.block, part.block).at[:, cols], buf["r"].at[k]) for k, who in enumerate((at.mate, at.far_mate))]
            else:
                pairs, base = [(buf["s" if kind == "x" else "b"], buf[kind])], base + (2 if kind == "x" else 3)
            return [
                pltpu.make_async_remote_copy(src, dst, send.at[base + k], recv.at[base + k], device_id=at.to[kind], device_id_type=MESH)
                for k, (src, dst) in enumerate(pairs)
            ]

        def start(n, kind):
            for copy in transfer(n, kind):
                copy.start()

        def finish(n, kind):
            for copy in transfer(n, kind):
                copy.wait()

        def add(n, which):
            part, buf = parts[n], bufs[n]
            k = 1 if which == "s" else 0
            own = part_rows(ref[part.name], (at.far if k else at.me) * part.block, part.block).at[:, pl.ds(part.start, part.width)]
            sources = [own, buf["r"].at[k]] + ([] if k else [buf["x"]])
            size = part.block // 2

            def run(ins, out):
                loads = []
                for p in range(2):
                    loads.append([pltpu.make_async_copy(src.at[pl.ds(p * size, size)], ins.at[q, pl.ds(p * size, size)], add_sems.at[3 * p + q]) for q, src in enumerate(sources)])
                    for copy in loads[-1]:
                        copy.start()
                stores = []
                for p in range(2):
                    for copy in loads[p]:
                        copy.wait()
                    here = pl.ds(p * size, size)
                    out[here] = sum(ins[q, here].astype(F32) for q in range(len(sources))).astype(BF16)
                    stores.append(pltpu.make_async_copy(out.at[here], buf[which].at[here], add_sems.at[6 + p]))
                    stores[-1].start()
                for copy in stores:
                    copy.wait()

            pl.run_scoped(run, pltpu.VMEM((len(sources), part.block, part.width), BF16), pltpu.VMEM((part.block, part.width), BF16))

        def to_x(n):
            finish(n, "mate")
            add(n, "s")
            start(n, "x")

        def to_y(n):
            finish(n, "x")
            add(n, "b")
            start(n, "y")

        def stage(body, steps, in_specs, out_specs, arrays, residents, events=None):
            def run(*scratch):
                copies, pairs = [], []
                for name, space in zip(residents, scratch, strict=True):
                    if name in matrices:
                        pairs.append((matrices[name].pairs(weight[name]), space))
                    else:
                        copies.append(pltpu.make_async_copy(ref[name], space, load_sems.at[len(copies)]))
                        copies[-1].start()
                copies += load(pairs, load_sems, len(copies))
                for copy in copies:
                    copy.wait()

                def inner(*blocks):
                    for when, what in (events or {}).items():

                        @pl.when(pl.program_id(0) == min(when, steps - 1))
                        def _():
                            for act, n in what:
                                act(n)

                    body(scratch, *blocks)

                pltpu.emit_pipeline(inner, grid=(steps,), in_specs=in_specs, out_specs=out_specs)(*(ref[name] for name in arrays))

            shapes_here = [matrices[name].shape if name in matrices else plain[name].shape if name in plain else made[name].shape for name in residents]
            pl.run_scoped(run, *[pltpu.VMEM(shape, BF16) for shape in shapes_here])

        def grad_in(a, b, out, events=None):
            def body(scratch, b_ref, o_ref):
                o_ref[...] = dot_tn(scratch[0][...], b_ref[...]).astype(BF16)

            stage(body, ff // col, [pl.BlockSpec((tokens, col), lambda i: (0, i))], [pl.BlockSpec((d, col), lambda i: (0, i))], (b, out), (a,), events)

        def grad_out(hidden, dres, out, events=None):
            def body(scratch, h_ref, o_ref):
                o_ref[...] = dot_tn(h_ref[...], scratch[0][...]).astype(BF16)

            stage(body, ff // col, [pl.BlockSpec((tokens, col), lambda i: (0, i))], [pl.BlockSpec((col, d), lambda i: (i, 0))], (hidden, out), (dres,), events)

        def input_back(dg, du, h, dres, gate, up, out, events=None):
            def body(scratch, dg_ref, du_ref, h_ref, r_ref, o_ref):
                da = rounded(rounded(dot_nt(dg_ref[...], scratch[0][...])) + rounded(dot_nt(du_ref[...], scratch[1][...])))
                o_ref[...] = norm_back(da, h_ref[...].astype(F32), r_ref[...].astype(F32))

            wide, narrow = pl.BlockSpec((tile, ff), lambda i: (i, 0)), pl.BlockSpec((tile, d), lambda i: (i, 0))
            stage(body, tokens // tile, [wide, wide, narrow, narrow], [narrow], (dg, du, h, dres, out), (gate, up), events)

        def hidden_back(events=None):
            size = min(256, ff)

            def body(scratch, h_ref, s_ref, q_ref, w_ref, dg_ref, du_ref):
                dres, wd = scratch
                w_ref[...] = dot_tn(h_ref[...], dres[...]).astype(BF16)
                here = pl.ds(pl.multiple_of(pl.program_id(0) * size, size), size)
                rows_at_once = min(512, tokens)

                @pl.loop(0, tokens // rows_at_once)
                def _(k):
                    some = pl.ds(pl.multiple_of(k * rows_at_once, rows_at_once), rows_at_once)
                    dh = rounded(dot_nt(dres[some], wd[here]))
                    dg_ref[some] = (dh * q_ref[some]).astype(BF16)
                    du_ref[some] = (dh * s_ref[some]).astype(BF16)

            tall = pl.BlockSpec((tokens, size), lambda i: (0, i))
            stage(
                body,
                ff // size,
                [tall] * 3,
                [pl.BlockSpec((size, d), lambda i: (i, 0)), tall, tall],
                ("hidden0", "silu", "slope", "wd0", "dg0", "du0"),
                ("dh", "down0"),
                events,
            )

        at.greet(("mate", "x", "y"))
        grad_out("hidden1", "dy", "wd1")
        start(WD1, "mate")
        grad_in("a1", "dg1", "wg1", {2: [(to_x, WD1)]})
        start(WG1, "mate")
        grad_in("a1", "du1", "wu1", {2: [(to_x, WG1)], 4: [(to_y, WD1)]})
        start(WU1, "mate")
        input_back("dg1", "du1", "h1", "dy", "gate1", "up1", "dh", {3: [(to_x, WU1)], 5: [(to_y, WG1)], 14: [(to_y, WU1)]})
        hidden_back()
        start(WD0, "mate")
        grad_in("a0", "dg0", "wg0", {2: [(to_x, WD0)]})
        start(WG0, "mate")
        grad_in("a0", "du0", "wu0", {2: [(to_x, WG0)], 4: [(to_y, WD0)]})
        start(WU0, "mate")
        start(WU0B, "mate")
        input_back(
            "dg0", "du0", "x", "dh", "gate0", "up0", "dx", {3: [(to_x, WU0), (to_x, WU0B)], 5: [(to_y, WG0)], 10: [(to_y, WU0)], 13: [(to_y, WU0B)]}
        )
        for n in range(len(parts)):
            finish(n, "y")

    results = pl.pallas_call(
        kernel,
        cost_estimate=cost(26 * tokens * d * ff),
        compiler_params=pltpu.CompilerParams(vmem_limit_bytes=62 << 20, collective_id=2, has_side_effects=True),
        in_specs=[ANY] * len(operands),
        out_specs=[ANY] * len(out_shape),
        out_shape=out_shape,
        scratch_shapes=[
            pltpu.SemaphoreType.DMA((4 * len(parts),)),
            pltpu.SemaphoreType.DMA((4 * len(parts),)),
            pltpu.SemaphoreType.DMA((40,)),
            pltpu.SemaphoreType.DMA((8,)),
        ],
        name="backward",
    )(*operands)
    dx = results[0]
    sums = {}
    results = results[len(made) :]
    for n, part in enumerate(parts):
        group = dict(zip(part_arrays[n], results[5 * n : 5 * n + 5], strict=True))
        sums.setdefault(part.name, []).append((group["b"], group["y"]))
    return dx, sums


def total(*terms):
    return sum(t.astype(F32) for t in terms).astype(BF16)


def solution(mesh):
    def step(x, dy, w_gate, w_up, w_down):
        x, dy = x[0], dy[0]
        weights = {"g": w_gate, "u": w_up, "d": w_down}
        (silu, slope, hidden0, a0), gathered = first_kernel(x, weights)

        def whole(name, layer):
            units, buffers = zip(*gathered[name, layer], strict=True)
            return Whole(weights[name], units, buffers)

        gate0, up0, down0 = (whole(name, 0) for name in "gud")
        (h1, a1), rest = second_kernel(hidden0, x, down0, weights)
        for unit, buf in rest:
            gathered.setdefault((unit.name, unit.layer), []).append((unit, buf))
        gate1, up1, down1 = (whole(name, 1) for name in "gud")
        hidden1, dg1, du1 = last_layer(a1, dy, gate1, up1, down1)
        dx, sums = backward(x, dy, a0, a1, h1, hidden0, hidden1, silu, slope, dg1, du1, gate0, up0, down0, gate1, up1)

        def out(name):
            return jnp.stack([jnp.concatenate([total(*pair) for pair in sums[name + layer]], 1) for layer in "01"])

        return dx[None], out("wg"), out("wu"), out("wd")

    states, cut = P(("rep", "r", "s"), None, None), P(None, "s", None)
    return jax.shard_map(
        step,
        mesh=mesh,
        in_specs=(states, states) + (cut,) * 3,
        out_specs=(states,) + (P("rep", "s", None),) * 3,
        check_vma=False,
    )
```

```python
import jax
import jax.numpy as jnp
from jax import lax
from jax.experimental import pallas as pl
from jax.experimental.pallas import tpu as pltpu
from jax.sharding import PartitionSpec as P

F32, BF16 = jnp.float32, jnp.bfloat16
ANY = pl.BlockSpec(memory_space=pl.ANY)
MESH = pl.DeviceIdType.MESH
NT = (((1,), (1,)), ((), ()))
TN = (((0,), (0,)), ((), ()))


def dot(a, b):
    return jnp.dot(a, b, preferred_element_type=F32)


def dot_nt(a, b):
    return lax.dot_general(a, b, NT, preferred_element_type=F32)


def dot_tn(a, b):
    return lax.dot_general(a, b, TN, preferred_element_type=F32)


def rounded(v):
    return v.astype(BF16).astype(F32)


def sigmoid(g):
    return pl.reciprocal(1.0 + jnp.exp(-g))


def normed(wide):
    return wide * lax.rsqrt(jnp.mean(wide * wide, -1, keepdims=True) + 1e-6)


def shaped(*shape, dtype=BF16):
    return jax.ShapeDtypeStruct(shape, dtype)


class Place:
    def __init__(self):
        self.me, self.y = lax.axis_index("s"), lax.axis_index("r")
        x, c = self.me // 2, self.me % 2
        self.mate, self.far, self.far_mate = 2 * x + 1 - c, 2 * (1 - x) + c, 2 * (1 - x) + 1 - c
        self.to = {"mate": {"s": self.mate}, "x": {"s": self.far}, "y": {"r": 1 - self.y}}

    def greet(self, whom):
        barrier = pltpu.get_barrier_semaphore()
        for name in whom:
            pl.semaphore_signal(barrier, inc=1, device_id=self.to[name], device_id_type=MESH)
        pl.semaphore_wait(barrier, len(whom))


def part_rows(ref, start, size):
    return ref.at[pl.ds(pl.multiple_of(start, 16), size)]


class Unit:
    def __init__(self, name, layer, start, width):
        self.name, self.layer, self.start, self.width = name, layer, start, width


class Mover:
    KINDS = ("own", "x", "y", "straight", "around")

    def __init__(self, units, weights, buffers, send, recv):
        self.units, self.weights, self.buffers, self.send, self.recv = units, weights, buffers, send, recv
        self.at = Place()

    def copy(self, n, kind, arriving=False):
        unit, buf, at = self.units[n], self.buffers[n], self.at
        block = buf.shape[0] // 4
        half = block // 2
        w = self.weights[unit.name].at[unit.layer]
        cols = pl.ds(unit.start, unit.width)
        mine, other = at.y * half, (1 - at.y) * half
        if arriving:
            start, size = {
                "own": (at.mate * block, block),
                "x": (at.far * block + mine, half),
                "y": (at.far * block + other, half),
                "straight": (at.far_mate * block + mine, half),
                "around": (at.far_mate * block + other, half),
            }[kind]
            src = dst = part_rows(buf, start, size)
        elif kind == "own":
            src, dst = w.at[:, cols], part_rows(buf, at.me * block, block)
        elif kind == "x":
            src, dst = w.at[pl.ds(pl.multiple_of(mine, 16), half), cols], part_rows(buf, at.me * block + mine, half)
        else:
            src = dst = part_rows(buf, at.far * block + (other if kind == "around" else mine), half)
        k = self.KINDS.index(kind)
        to = at.to[{"x": "x", "y": "y"}.get(kind, "mate")]
        return pltpu.make_async_remote_copy(src, dst, self.send.at[n, k], self.recv.at[n, k], device_id=to, device_id_type=MESH)

    def start(self, ns, *kinds):
        for n in ns:
            for kind in kinds:
                self.copy(n, kind).start()

    def arrived(self, ns, *kinds):
        for n in ns:
            for kind in kinds:
                self.copy(n, kind, arriving=True).wait_recv()

    def sent(self, ns):
        for n in ns:
            for kind in self.KINDS:
                self.copy(n, kind).wait_send()


def load(pairs, sems, first=0):
    at, made = Place(), []
    for units, scratch in pairs:
        col = 0
        for unit, w, buf in units:
            block = buf.shape[0] // 4
            for n, who in enumerate((at.me, at.mate, at.far, at.far_mate)):
                src = w.at[unit.layer, :, pl.ds(unit.start, unit.width)] if n == 0 else part_rows(buf, who * block, block)
                dst = scratch.at[pl.ds(pl.multiple_of(who * block, 16), block), pl.ds(col, unit.width)]
                made.append(pltpu.make_async_copy(src, dst, sems.at[first + len(made)]))
                made[-1].start()
            col += unit.width
    return made


def norm_back(da, wide, dres):
    scale = lax.rsqrt(jnp.mean(wide * wide, -1, keepdims=True) + 1e-6)
    along = jnp.sum(da * wide, -1, keepdims=True) * (scale * scale * scale) * (1.0 / wide.shape[-1])
    return (dres + rounded(da * scale - wide * along)).astype(BF16)


class Part:
    def __init__(self, name, term_shape, start, width):
        self.name, self.start, self.width = name, start, width
        self.block = term_shape[0] // 4

    def arrays(self):
        one = shaped(self.block, self.width)
        return {"r": shaped(2, self.block, self.width), "s": one, "x": one, "b": one, "y": one}


def everything(x, dy, weights):
    tokens, d = x.shape
    ff = weights["g"].shape[2]
    block = ff // 4
    shapes = {"wg": (d, ff), "wu": (d, ff), "wd": (ff, d)}
    terms = {name + layer: shaped(*shapes[name]) for layer in "10" for name in ("wd", "wg", "wu")}
    parts = [Part(name, terms[name].shape, 0, terms[name].shape[1]) for name in ("wd1", "wg1", "wu1")]
    for name in ("wd0", "wg0", "wu0"):
        width = terms[name].shape[1] // 2
        parts += [Part(name, terms[name].shape, n * width, width) for n in range(2)]
    WD1, WG1, WU1, WD0A, WD0B, WG0A, WG0B, WU0A, WU0B = range(9)
    units, groups = [], []
    for c in range(4):
        groups.append((len(units), len(units) + 1))
        units += [Unit("g", 0, c * block, block), Unit("u", 0, c * block, block)]
    for name, layer in (("d", 0), ("g", 1), ("u", 1), ("d", 1)):
        columns = weights[name].shape[2] // 2
        for n in range(2):
            groups.append((len(units),))
            units.append(Unit(name, layer, n * columns, columns))
    of = {}
    for n, unit in enumerate(units):
        of.setdefault(unit.name + str(unit.layer), []).append(n)
    states, wide = shaped(tokens, d), shaped(tokens, ff)
    made = {name: states for name in ("dx", "dh", "a0", "a1", "h1")} | {name: wide for name in ("hidden0", "hidden1", "dg0", "du0", "dg1", "du1")}
    made |= {name: shaped(tokens, ff, dtype=F32) for name in ("silu", "slope")} | {name: shaped(tokens, block) for name in ("early0", "early1")} | terms
    part_arrays = [part.arrays() for part in parts]
    buffer_shapes = [shaped(4 * weights[unit.name].shape[1], unit.width) for unit in units]
    out_shape = list(made.values()) + buffer_shapes + [one for group in part_arrays for one in group.values()]
    tile = min(256, tokens)
    col = min(512, ff)

    def kernel(*refs):
        refs = list(refs)

        def take(n):
            taken, refs[:] = refs[:n], refs[n:]
            return taken

        ref = dict(zip(("x", "dy"), take(2), strict=True))
        weight = dict(zip(weights, take(len(weights)), strict=True))
        ref.update(zip(made, take(len(made)), strict=True))
        buffers = take(len(units))
        bufs = [dict(zip(group, take(len(group)), strict=True)) for group in part_arrays]
        send, recv, load_sems, add_sems, unit_send, unit_recv = refs
        move = Mover(units, weight, buffers, unit_send, unit_recv)
        at = move.at

        def over_x(k):
            move.arrived(groups[k], "x")
            move.start(groups[k], "y", "straight")
            if k + 2 < len(groups):
                move.start(groups[k + 2], "x")

        def over_y(k):
            move.arrived(groups[k], "y")
            move.start(groups[k], "around")

        def arrived(*ks):
            for k in ks:
                move.arrived(groups[k], "own", "straight", "around")

        def transfer(n, kind):
            part, buf = parts[n], bufs[n]
            base = 4 * n
            if kind == "mate":
                cols = pl.ds(part.start, part.width)
                pairs = [(part_rows(ref[part.name], who * part.block, part.block).at[:, cols], buf["r"].at[k]) for k, who in enumerate((at.mate, at.far_mate))]
            else:
                pairs, base = [(buf["s" if kind == "x" else "b"], buf[kind])], base + (2 if kind == "x" else 3)
            return [
                pltpu.make_async_remote_copy(src, dst, send.at[base + k], recv.at[base + k], device_id=at.to[kind], device_id_type=MESH)
                for k, (src, dst) in enumerate(pairs)
            ]

        def start(n, kind):
            for copy in transfer(n, kind):
                copy.start()

        def finish(n, kind):
            for copy in transfer(n, kind):
                copy.wait()

        def sources(n, which):
            part, buf = parts[n], bufs[n]
            own = part_rows(ref[part.name], (at.far if which == "s" else at.me) * part.block, part.block).at[:, pl.ds(part.start, part.width)]
            return [own, buf["r"].at[1]] if which == "s" else [own, buf["r"].at[0], buf["x"]]

        def sum_loads(n, which, space):
            base = 10 * n + (5 if which == "b" else 0)
            return [pltpu.make_async_copy(src, space.at[q], add_sems.at[base + q]) for q, src in enumerate(sources(n, which))]

        def before_sum(n, which, space):
            finish(n, "mate" if which == "s" else "x")
            for copy in sum_loads(n, which, space):
                copy.start()

        def sum_and_send(n, which, space):
            for copy in sum_loads(n, which, space):
                copy.wait()
            part, stores = parts[n], []
            size = part.block // 2
            for p in range(2):
                here = pl.ds(p * size, size)
                space[0, here] = sum(space[q, here].astype(F32) for q in range(space.shape[0])).astype(BF16)
                stores.append(pltpu.make_async_copy(space.at[0, here], bufs[n][which].at[here], add_sems.at[10 * n + (5 if which == "b" else 0) + 3 + p]))
                stores[-1].start()
            for copy in stores:
                copy.wait()
            start(n, "x" if which == "s" else "y")

        def stage(body, steps, in_specs, out_specs, arrays, residents, events=(), acts=()):
            events = [(min(when, steps - 1), min(when + 1, steps - 1), n, which) for when, n, which in events]

            def run(*scratch):
                scratch, spaces = scratch[: len(residents)], scratch[len(residents) :]
                copies, pairs = [], []
                for what, space in zip(residents, scratch, strict=True):
                    if isinstance(what, str):
                        copies.append(pltpu.make_async_copy(ref[what], space, load_sems.at[len(copies)]))
                        copies[-1].start()
                    else:
                        pairs.append(([(units[n], weight[units[n].name], buffers[n]) for n in what], space))
                copies += load(pairs, load_sems, len(copies))
                for copy in copies:
                    copy.wait()

                def inner(*blocks):
                    now = pl.program_id(0)
                    for (first, then, n, which), space in zip(events, spaces, strict=True):

                        @pl.when(now == first)
                        def _():
                            before_sum(n, which, space)

                        @pl.when(now == then)
                        def _():
                            sum_and_send(n, which, space)

                    for when, act, k in acts:

                        @pl.when(now == min(when, steps - 1))
                        def _():
                            act(k)

                    body(scratch, *blocks)

                pltpu.emit_pipeline(inner, grid=(steps,), in_specs=in_specs, out_specs=out_specs)(*(ref[name] for name in arrays))

            shapes_here = [
                ref[what].shape if isinstance(what, str) else (buffer_shapes[what[0]].shape[0], sum(units[n].width for n in what)) for what in residents
            ]
            shapes_here += [(2 if which == "s" else 3, parts[n].block, parts[n].width) for *_, n, which in events]
            pl.run_scoped(run, *[pltpu.VMEM(shape, BF16) for shape in shapes_here])

        def grad_in(a, b, out, events=()):
            def body(scratch, b_ref, o_ref):
                o_ref[...] = dot_tn(scratch[0][...], b_ref[...]).astype(BF16)

            stage(body, ff // col, [pl.BlockSpec((tokens, col), lambda i: (0, i))], [pl.BlockSpec((d, col), lambda i: (0, i))], (b, out), (a,), events)

        def grad_out(hidden, dres, out, events=()):
            def body(scratch, h_ref, o_ref):
                o_ref[...] = dot_tn(h_ref[...], scratch[0][...]).astype(BF16)

            stage(body, ff // col, [pl.BlockSpec((tokens, col), lambda i: (0, i))], [pl.BlockSpec((col, d), lambda i: (i, 0))], (hidden, out), (dres,), events)

        def input_back(dg, du, h, dres, gate, up, out, events=()):
            def body(scratch, dg_ref, du_ref, h_ref, r_ref, o_ref):
                da = rounded(rounded(dot_nt(dg_ref[...], scratch[0][...])) + rounded(dot_nt(du_ref[...], scratch[1][...])))
                o_ref[...] = norm_back(da, h_ref[...].astype(F32), r_ref[...].astype(F32))

            wide, narrow = pl.BlockSpec((tile, ff), lambda i: (i, 0)), pl.BlockSpec((tile, d), lambda i: (i, 0))
            stage(body, tokens // tile, [wide, wide, narrow, narrow], [narrow], (dg, du, h, dres, out), (of[gate], of[up]), events)

        def hidden_back(events=()):
            size = min(256, ff)

            def body(scratch, h_ref, s_ref, q_ref, w_ref, dg_ref, du_ref):
                dres, wd = scratch
                w_ref[...] = dot_tn(h_ref[...], dres[...]).astype(BF16)
                here = pl.ds(pl.multiple_of(pl.program_id(0) * size, size), size)
                rows_at_once = min(512, tokens)

                @pl.loop(0, tokens // rows_at_once)
                def _(k):
                    some = pl.ds(pl.multiple_of(k * rows_at_once, rows_at_once), rows_at_once)
                    dh = rounded(dot_nt(dres[some], wd[here]))
                    dg_ref[some] = (dh * q_ref[some]).astype(BF16)
                    du_ref[some] = (dh * s_ref[some]).astype(BF16)

            tall = pl.BlockSpec((tokens, size), lambda i: (0, i))
            stage(
                body,
                ff // size,
                [tall] * 3,
                [pl.BlockSpec((size, d), lambda i: (i, 0)), tall, tall],
                ("hidden0", "silu", "slope", "wd0", "dg0", "du0"),
                ("dh", of["d0"]),
                events,
            )

        wide_tile, narrow_tile = pl.BlockSpec((tile, ff), lambda i: (i, 0)), pl.BlockSpec((tile, d), lambda i: (i, 0))
        early_tile = pl.BlockSpec((tile, block), lambda i: (i, 0))
        big = min(512, tokens)

        def early(which, acts):
            def run(space):
                if which:
                    move.arrived(of["d1"], "own")
                    copies, at_col = [], 0
                    for n in of["d1"]:
                        copies.append((part_rows(buffers[n], at.mate * block, block), space.at[:, pl.ds(at_col, units[n].width)]))
                        at_col += units[n].width
                else:
                    copies = [(weight["d"].at[1], space)]
                copies = [pltpu.make_async_copy(src, dst, load_sems.at[n]) for n, (src, dst) in enumerate(copies)]
                for copy in copies:
                    copy.start()
                for copy in copies:
                    copy.wait()

                def body(dy_ref, o_ref, *more):
                    for when, act, k in acts:

                        @pl.when(pl.program_id(0) == min(when, tokens // big - 1))
                        def _():
                            act(k)

                    o_ref[...] = dot_nt(dy_ref[...], space[...]).astype(BF16)

                one, out = pl.BlockSpec((big, d), lambda i: (i, 0)), pl.BlockSpec((big, block), lambda i: (i, 0))
                pltpu.emit_pipeline(body, grid=(tokens // big,), in_specs=[one], out_specs=[out])(ref["dy"], ref[f"early{which}"])

            pl.run_scoped(run, pltpu.VMEM((block, d), BF16))

        def norm_x():
            def body(x_ref, a_ref):
                a_ref[...] = normed(x_ref[...].astype(F32)).astype(BF16)

            one = pl.BlockSpec((big, d), lambda i: (i, 0))
            pltpu.emit_pipeline(body, grid=(tokens // big,), in_specs=[one], out_specs=[one])(ref["x"], ref["a0"])

        def gate_up(first, count, acts):
            width, size = count * block, min(256, block)

            def body(scratch, a_ref, s_ref, q_ref, h_ref):
                wg, wu = scratch
                av = a_ref[...]
                for j in range(0, width, size):
                    here = pl.ds(j, size)
                    g, u = dot(av, wg[:, here]), dot(av, wu[:, here])
                    s = sigmoid(g)
                    sl = g * s
                    s_ref[:, here] = sl
                    q_ref[:, here] = u * (s + sl * (1.0 - s))
                    h_ref[:, here] = (sl * u).astype(BF16)

            out = pl.BlockSpec((big, width), lambda i: (i, first // count))
            weights_here = tuple(of[name][first : first + count] for name in ("g0", "u0"))
            stage(body, tokens // big, [pl.BlockSpec((big, d), lambda i: (i, 0))], [out] * 3, ("a0", "silu", "slope", "hidden0"), weights_here, (), acts)

        def down(acts):
            def body(scratch, hidden_ref, x_ref, h_ref, a_ref):
                out = (x_ref[...].astype(F32) + rounded(dot(hidden_ref[...], scratch[0][...]))).astype(BF16)
                h_ref[...] = out
                a_ref[...] = normed(out.astype(F32)).astype(BF16)

            stage(body, tokens // tile, [wide_tile, narrow_tile], [narrow_tile] * 2, ("hidden0", "x", "h1", "a1"), (of["d0"],), (), acts)

        def last_layer():
            size = min(256, block)

            def body(scratch, a_ref, dy_ref, e0_ref, e1_ref, h_ref, dg_ref, du_ref):
                wg, wu, wd = scratch
                av, dyv = a_ref[...], dy_ref[...]
                for q, who in enumerate((at.me, at.mate, at.far, at.far_mate)):
                    for j in range(0, block, size):
                        here = pl.ds(pl.multiple_of(who * block + j, size), size)
                        g, u = dot(av, wg[:, here]), dot(av, wu[:, here])
                        dh = (e0_ref, e1_ref)[q][:, pl.ds(j, size)].astype(F32) if q < 2 else rounded(dot_nt(dyv, wd[here, :]))
                        s = sigmoid(g)
                        sl = g * s
                        h_ref[:, here] = (sl * u).astype(BF16)
                        dg_ref[:, here] = (dh * (u * (s + sl * (1.0 - s)))).astype(BF16)
                        du_ref[:, here] = (dh * sl).astype(BF16)

            specs = [narrow_tile] * 2 + [early_tile] * 2
            arrays = ("a1", "dy", "early0", "early1", "hidden1", "dg1", "du1")
            stage(body, tokens // tile, specs, [wide_tile] * 3, arrays, (of["g1"], of["u1"], of["d1"]))

        at.greet(("mate", "x", "y"))
        move.start(groups[0] + groups[1], "x")
        move.start(of["d1"], "own")
        for group in groups[:-2]:
            move.start(group, "own")
        early(0, ())
        norm_x()
        early(1, [(1, over_x, 0)])
        over_x(1)
        over_y(0)
        arrived(0)
        gate_up(0, 1, [(3, over_x, 2), (3, over_y, 1), (7, over_x, 3), (7, over_y, 2)])
        arrived(1)
        gate_up(1, 1, [(3, over_x, 4), (3, over_y, 3), (7, over_x, 5), (7, over_y, 4)])
        arrived(2, 3)
        gate_up(2, 2, [(2, over_x, 6), (2, over_y, 5), (4, over_x, 7), (4, over_y, 6), (6, over_x, 8), (6, over_y, 7)])
        arrived(4, 5)
        down([(0, over_x, 9), (0, over_y, 8), (3, over_x, 10), (4, over_y, 9), (7, over_x, 11), (8, over_y, 10), (12, over_y, 11)])
        arrived(6, 7, 8, 9)
        for n in of["d1"]:
            move.arrived((n,), "straight", "around")
        last_layer()

        grad_out("hidden1", "dy", "wd1")
        start(WD1, "mate")
        grad_in("a1", "dg1", "wg1", [(2, WD1, "s")])
        start(WG1, "mate")
        grad_in("a1", "du1", "wu1", [(2, WG1, "s"), (4, WD1, "b")])
        start(WU1, "mate")
        input_back("dg1", "du1", "h1", "dy", "g1", "u1", "dh", [(2, WU1, "s"), (6, WG1, "b"), (14, WU1, "b")])
        hidden_back()
        start(WD0A, "mate")
        start(WD0B, "mate")
        grad_in("a0", "dg0", "wg0", [(1, WD0A, "s"), (1, WD0B, "s")])
        start(WG0A, "mate")
        start(WG0B, "mate")
        grad_in("a0", "du0", "wu0", [(0, WD0A, "b"), (1, WG0A, "s"), (1, WG0B, "s"), (3, WD0B, "b")])
        start(WU0A, "mate")
        start(WU0B, "mate")
        late = [(0, WG0A, "b"), (2, WU0A, "s"), (2, WU0B, "s"), (5, WG0B, "b"), (10, WU0A, "b"), (14, WU0B, "b")]
        input_back("dg0", "du0", "x", "dh", "g0", "u0", "dx", late)
        move.sent(range(len(units)))
        for n in range(len(parts)):
            finish(n, "y")

    results = pl.pallas_call(
        kernel,
        cost_estimate=pl.CostEstimate(flops=34 * tokens * d * ff, bytes_accessed=1 << 30, transcendentals=0),
        compiler_params=pltpu.CompilerParams(vmem_limit_bytes=62 << 20, collective_id=0, has_side_effects=True),
        in_specs=[ANY] * (2 + len(weights)),
        out_specs=[ANY] * len(out_shape),
        out_shape=out_shape,
        scratch_shapes=[
            pltpu.SemaphoreType.DMA((4 * len(parts),)),
            pltpu.SemaphoreType.DMA((4 * len(parts),)),
            pltpu.SemaphoreType.DMA((40,)),
            pltpu.SemaphoreType.DMA((10 * len(parts),)),
            pltpu.SemaphoreType.DMA((len(units), 5)),
            pltpu.SemaphoreType.DMA((len(units), 5)),
        ],
        name="layers",
    )(x, dy, *weights.values())
    dx = results[0]
    sums = {}
    results = results[len(made) + len(units) :]
    for n, part in enumerate(parts):
        group = dict(zip(part_arrays[n], results[5 * n : 5 * n + 5], strict=True))
        sums.setdefault(part.name, []).append((group["b"], group["y"]))
    return dx, sums


def total(*terms):
    return sum(t.astype(F32) for t in terms).astype(BF16)


def solution(mesh):
    def step(x, dy, w_gate, w_up, w_down):
        x, dy = x[0], dy[0]
        weights = {"g": w_gate, "u": w_up, "d": w_down}
        dx, sums = everything(x, dy, weights)

        def out(name):
            return jnp.stack([jnp.concatenate([total(*pair) for pair in sums[name + layer]], 1) for layer in "01"])

        return dx[None], out("wg"), out("wu"), out("wd")

    states, cut = P(("rep", "r", "s"), None, None), P(None, "s", None)
    return jax.shard_map(
        step,
        mesh=mesh,
        in_specs=(states, states) + (cut,) * 3,
        out_specs=(states,) + (P("rep", "s", None),) * 3,
        check_vma=False,
    )
```

```python
import jax
import jax.numpy as jnp
from jax import lax
from jax.experimental import pallas as pl
from jax.experimental.pallas import tpu as pltpu
from jax.sharding import PartitionSpec as P

F32, BF16 = jnp.float32, jnp.bfloat16
ANY = pl.BlockSpec(memory_space=pl.ANY)
MESH = pl.DeviceIdType.MESH
NT = (((1,), (1,)), ((), ()))
TN = (((0,), (0,)), ((), ()))


def dot(a, b):
    return jnp.dot(a, b, preferred_element_type=F32)


def dot_nt(a, b):
    return lax.dot_general(a, b, NT, preferred_element_type=F32)


def dot_tn(a, b):
    return lax.dot_general(a, b, TN, preferred_element_type=F32)


def rounded(v):
    return v.astype(BF16).astype(F32)


def sigmoid(g):
    return pl.reciprocal(1.0 + jnp.exp(-g))


def normed(wide):
    return wide * lax.rsqrt(jnp.mean(wide * wide, -1, keepdims=True) + 1e-6)


def shaped(*shape, dtype=BF16):
    return jax.ShapeDtypeStruct(shape, dtype)


class Place:
    def __init__(self):
        self.me, self.y = lax.axis_index("s"), lax.axis_index("r")
        x, c = self.me // 2, self.me % 2
        self.mate, self.far, self.far_mate = 2 * x + 1 - c, 2 * (1 - x) + c, 2 * (1 - x) + 1 - c
        self.to = {"mate": {"s": self.mate}, "x": {"s": self.far}, "y": {"r": 1 - self.y}}

    def greet(self, whom):
        barrier = pltpu.get_barrier_semaphore()
        for name in whom:
            pl.semaphore_signal(barrier, inc=1, device_id=self.to[name], device_id_type=MESH)
        pl.semaphore_wait(barrier, len(whom))


def part_rows(ref, start, size):
    return ref.at[pl.ds(pl.multiple_of(start, 16), size)]


class Unit:
    def __init__(self, name, layer, start, width):
        self.name, self.layer, self.start, self.width = name, layer, start, width


class Mover:
    KINDS = ("own", "x", "y", "straight", "around")

    def __init__(self, units, weights, buffers, send, recv):
        self.units, self.weights, self.buffers, self.send, self.recv = units, weights, buffers, send, recv
        self.at = Place()

    def copy(self, n, kind, arriving=False):
        unit, buf, at = self.units[n], self.buffers[n], self.at
        block = buf.shape[0] // 4
        half = block // 2
        w = self.weights[unit.name].at[unit.layer]
        cols = pl.ds(unit.start, unit.width)
        mine, other = at.y * half, (1 - at.y) * half
        if arriving:
            start, size = {
                "own": (at.mate * block, block),
                "x": (at.far * block + mine, half),
                "y": (at.far * block + other, half),
                "straight": (at.far_mate * block + mine, half),
                "around": (at.far_mate * block + other, half),
            }[kind]
            src = dst = part_rows(buf, start, size)
        elif kind == "own":
            src, dst = w.at[:, cols], part_rows(buf, at.me * block, block)
        elif kind == "x":
            src, dst = w.at[pl.ds(pl.multiple_of(mine, 16), half), cols], part_rows(buf, at.me * block + mine, half)
        else:
            src = dst = part_rows(buf, at.far * block + (other if kind == "around" else mine), half)
        k = self.KINDS.index(kind)
        to = at.to[{"x": "x", "y": "y"}.get(kind, "mate")]
        return pltpu.make_async_remote_copy(src, dst, self.send.at[n, k], self.recv.at[n, k], device_id=to, device_id_type=MESH)

    def start(self, ns, *kinds):
        for n in ns:
            for kind in kinds:
                self.copy(n, kind).start()

    def arrived(self, ns, *kinds):
        for n in ns:
            for kind in kinds:
                self.copy(n, kind, arriving=True).wait_recv()

    def sent(self, ns):
        for n in ns:
            for kind in self.KINDS:
                self.copy(n, kind).wait_send()


def load(pairs, sems, first=0):
    at, made = Place(), []
    for units, scratch in pairs:
        col = 0
        for unit, w, buf in units:
            block = buf.shape[0] // 4
            for n, who in enumerate((at.me, at.mate, at.far, at.far_mate)):
                src = w.at[unit.layer, :, pl.ds(unit.start, unit.width)] if n == 0 else part_rows(buf, who * block, block)
                dst = scratch.at[pl.ds(pl.multiple_of(who * block, 16), block), pl.ds(col, unit.width)]
                made.append(pltpu.make_async_copy(src, dst, sems.at[first + len(made)]))
                made[-1].start()
            col += unit.width
    return made


def norm_back(da, wide, dres):
    scale = lax.rsqrt(jnp.mean(wide * wide, -1, keepdims=True) + 1e-6)
    along = jnp.sum(da * wide, -1, keepdims=True) * (scale * scale * scale) * (1.0 / wide.shape[-1])
    return (dres + rounded(da * scale - wide * along)).astype(BF16)


class Part:
    def __init__(self, name, term_shape, start, width):
        self.name, self.start, self.width = name, start, width
        self.block = term_shape[0] // 4

    def arrays(self):
        one = shaped(self.block, self.width)
        return {"r": shaped(2, self.block, self.width), "s": one, "x": one, "b": one, "y": one}


def everything(x, dy, weights):
    tokens, d = x.shape
    ff = weights["g"].shape[2]
    block = ff // 4
    shapes = {"wg": (d, ff), "wu": (d, ff), "wd": (ff, d)}
    terms = {name + layer: shaped(*shapes[name]) for layer in "10" for name in ("wd", "wg", "wu")}
    parts = [Part(name, terms[name].shape, 0, terms[name].shape[1]) for name in ("wd1", "wg1", "wu1")]
    for name in ("wd0", "wg0", "wu0"):
        width = terms[name].shape[1] // 2
        parts += [Part(name, terms[name].shape, n * width, width) for n in range(2)]
    WD1, WG1, WU1, WD0A, WD0B, WG0A, WG0B, WU0A, WU0B = range(9)
    units, groups = [], []
    for c in range(4):
        groups.append((len(units), len(units) + 1))
        units += [Unit("g", 0, c * block, block), Unit("u", 0, c * block, block)]
    for name, layer in (("d", 0), ("g", 1), ("u", 1), ("d", 1)):
        columns = weights[name].shape[2] // 2
        for n in range(2):
            groups.append((len(units),))
            units.append(Unit(name, layer, n * columns, columns))
    of = {}
    for n, unit in enumerate(units):
        of.setdefault(unit.name + str(unit.layer), []).append(n)
    states, wide = shaped(tokens, d), shaped(tokens, ff)
    made = {name: states for name in ("dx", "dh", "a0", "a1", "h1")} | {name: wide for name in ("hidden0", "hidden1", "dg0", "du0", "dg1", "du1")}
    made |= {name: shaped(tokens, ff, dtype=F32) for name in ("silu", "slope")} | {name: shaped(tokens, block) for name in ("early0", "early1")} | terms
    part_arrays = [part.arrays() for part in parts]
    buffer_shapes = [shaped(4 * weights[unit.name].shape[1], unit.width) for unit in units]
    out_shape = list(made.values()) + buffer_shapes + [one for group in part_arrays for one in group.values()]
    tile = min(256, tokens)
    col = min(512, ff)

    def kernel(*refs):
        refs = list(refs)

        def take(n):
            taken, refs[:] = refs[:n], refs[n:]
            return taken

        ref = dict(zip(("x", "dy"), take(2), strict=True))
        weight = dict(zip(weights, take(len(weights)), strict=True))
        ref.update(zip(made, take(len(made)), strict=True))
        buffers = take(len(units))
        bufs = [dict(zip(group, take(len(group)), strict=True)) for group in part_arrays]
        send, recv, load_sems, add_sems, unit_send, unit_recv = refs
        move = Mover(units, weight, buffers, unit_send, unit_recv)
        at = move.at

        def over_x(k):
            move.arrived(groups[k], "x")
            move.start(groups[k], "y", "straight")
            if k + 2 < len(groups):
                move.start(groups[k + 2], "x")

        def over_y(k):
            move.arrived(groups[k], "y")
            move.start(groups[k], "around")

        def arrived(*ks):
            for k in ks:
                move.arrived(groups[k], "own", "straight", "around")

        def transfer(n, kind):
            part, buf = parts[n], bufs[n]
            base = 4 * n
            if kind == "mate":
                cols = pl.ds(part.start, part.width)
                pairs = [(part_rows(ref[part.name], who * part.block, part.block).at[:, cols], buf["r"].at[k]) for k, who in enumerate((at.mate, at.far_mate))]
            else:
                pairs, base = [(buf["s" if kind == "x" else "b"], buf[kind])], base + (2 if kind == "x" else 3)
            return [
                pltpu.make_async_remote_copy(src, dst, send.at[base + k], recv.at[base + k], device_id=at.to[kind], device_id_type=MESH)
                for k, (src, dst) in enumerate(pairs)
            ]

        def start(n, kind):
            for copy in transfer(n, kind):
                copy.start()

        def finish(n, kind):
            for copy in transfer(n, kind):
                copy.wait()

        def sources(n, which):
            part, buf = parts[n], bufs[n]
            own = part_rows(ref[part.name], (at.far if which == "s" else at.me) * part.block, part.block).at[:, pl.ds(part.start, part.width)]
            return [own, buf["r"].at[1]] if which == "s" else [own, buf["r"].at[0], buf["x"]]

        def sum_loads(n, which, space):
            base = 10 * n + (5 if which == "b" else 0)
            return [pltpu.make_async_copy(src, space.at[q], add_sems.at[base + q]) for q, src in enumerate(sources(n, which))]

        def before_sum(n, which, space):
            finish(n, "mate" if which == "s" else "x")
            for copy in sum_loads(n, which, space):
                copy.start()

        def sum_and_send(n, which, space):
            for copy in sum_loads(n, which, space):
                copy.wait()
            part, stores = parts[n], []
            size = part.block // 2
            for p in range(2):
                here = pl.ds(p * size, size)
                space[0, here] = sum(space[q, here].astype(F32) for q in range(space.shape[0])).astype(BF16)
                stores.append(pltpu.make_async_copy(space.at[0, here], bufs[n][which].at[here], add_sems.at[10 * n + (5 if which == "b" else 0) + 3 + p]))
                stores[-1].start()
            for copy in stores:
                copy.wait()
            start(n, "x" if which == "s" else "y")

        def fetches(residents, scratch, base=0):
            copies, pairs = [], []
            for what, space in zip(residents, scratch, strict=True):
                if isinstance(what, str):
                    copies.append(pltpu.make_async_copy(ref[what], space, load_sems.at[base + len(copies)]))
                    copies[-1].start()
                else:
                    pairs.append(([(units[n], weight[units[n].name], buffers[n]) for n in what], space))
            return copies + load(pairs, load_sems, base + len(copies))

        def spaces_for(residents):
            return [
                pltpu.VMEM(ref[what].shape if isinstance(what, str) else (buffer_shapes[what[0]].shape[0], sum(units[n].width for n in what)), BF16)
                for what in residents
            ]

        def ahead(residents, before, after, base=40):
            def run(*scratch):
                copies = fetches(residents, scratch, base)
                before()
                for copy in copies:
                    copy.wait()
                after(scratch)

            pl.run_scoped(run, *spaces_for(residents))

        def stage(body, steps, in_specs, out_specs, arrays, residents, events=(), acts=(), ready=None):
            events = [(min(when, steps - 1), min(when + 1, steps - 1), n, which) for when, n, which in events]

            def run(*scratch):
                scratch, spaces = scratch[: len(residents)], scratch[len(residents) :]
                copies = fetches(residents, scratch)

                def inner(*blocks):
                    now = pl.program_id(0)
                    if copies:

                        @pl.when(now == 0)
                        def _():
                            for copy in copies:
                                copy.wait()

                    for (first, then, n, which), space in zip(events, spaces, strict=True):

                        @pl.when(now == first)
                        def _():
                            before_sum(n, which, space)

                        @pl.when(now == then)
                        def _():
                            sum_and_send(n, which, space)

                    for when, act, k in acts:

                        @pl.when(now == min(when, steps - 1))
                        def _():
                            act(k)

                    body(ready or scratch, *blocks)

                pltpu.emit_pipeline(inner, grid=(steps,), in_specs=in_specs, out_specs=out_specs)(*(ref[name] for name in arrays))

            sums = [pltpu.VMEM((2 if which == "s" else 3, parts[n].block, parts[n].width), BF16) for *_, n, which in events]
            if residents or sums:
                pl.run_scoped(run, *spaces_for(residents), *sums)
            else:
                run()

        def grad_in(a, b, out, events=()):
            def body(spaces, b_ref, o_ref):
                o_ref[...] = dot_tn(a[...], b_ref[...]).astype(BF16)

            stage(body, ff // col, [pl.BlockSpec((tokens, col), lambda i: (0, i))], [pl.BlockSpec((d, col), lambda i: (0, i))], (b, out), (), events)

        def grad_out(ready, hidden, out):
            def body(scratch, h_ref, o_ref):
                o_ref[...] = dot_tn(h_ref[...], scratch[0][...]).astype(BF16)

            stage(body, ff // col, [pl.BlockSpec((tokens, col), lambda i: (0, i))], [pl.BlockSpec((col, d), lambda i: (i, 0))], (hidden, out), (), ready=ready)

        def input_back(ready, dg, du, h, dres, out, events=()):
            def body(scratch, dg_ref, du_ref, h_ref, r_ref, o_ref):
                da = rounded(rounded(dot_nt(dg_ref[...], scratch[0][...])) + rounded(dot_nt(du_ref[...], scratch[1][...])))
                o_ref[...] = norm_back(da, h_ref[...].astype(F32), r_ref[...].astype(F32))

            wide, narrow = pl.BlockSpec((tile, ff), lambda i: (i, 0)), pl.BlockSpec((tile, d), lambda i: (i, 0))
            stage(body, tokens // tile, [wide, wide, narrow, narrow], [narrow], (dg, du, h, dres, out), (), events, ready=ready)

        def hidden_back(events=()):
            size = min(256, ff)

            def body(scratch, h_ref, s_ref, q_ref, w_ref, dg_ref, du_ref):
                dres, wd = scratch
                w_ref[...] = dot_tn(h_ref[...], dres[...]).astype(BF16)
                here = pl.ds(pl.multiple_of(pl.program_id(0) * size, size), size)
                rows_at_once = min(512, tokens)

                @pl.loop(0, tokens // rows_at_once)
                def _(k):
                    some = pl.ds(pl.multiple_of(k * rows_at_once, rows_at_once), rows_at_once)
                    dh = rounded(dot_nt(dres[some], wd[here]))
                    dg_ref[some] = (dh * q_ref[some]).astype(BF16)
                    du_ref[some] = (dh * s_ref[some]).astype(BF16)

            tall = pl.BlockSpec((tokens, size), lambda i: (0, i))
            stage(
                body,
                ff // size,
                [tall] * 3,
                [pl.BlockSpec((size, d), lambda i: (i, 0)), tall, tall],
                ("hidden0", "silu", "slope", "wd0", "dg0", "du0"),
                ("dh", of["d0"]),
                events,
            )

        wide_tile, narrow_tile = pl.BlockSpec((tile, ff), lambda i: (i, 0)), pl.BlockSpec((tile, d), lambda i: (i, 0))
        early_tile = pl.BlockSpec((tile, block), lambda i: (i, 0))
        big = min(512, tokens)

        def early(which, acts):
            def run(space):
                if which:
                    move.arrived(of["d1"], "own")
                    copies, at_col = [], 0
                    for n in of["d1"]:
                        copies.append((part_rows(buffers[n], at.mate * block, block), space.at[:, pl.ds(at_col, units[n].width)]))
                        at_col += units[n].width
                else:
                    copies = [(weight["d"].at[1], space)]
                copies = [pltpu.make_async_copy(src, dst, load_sems.at[n]) for n, (src, dst) in enumerate(copies)]
                for copy in copies:
                    copy.start()
                for copy in copies:
                    copy.wait()

                def body(*blocks):
                    for when, act, k in acts:

                        @pl.when(pl.program_id(0) == min(when, tokens // big - 1))
                        def _():
                            act(k)

                    if which:
                        dy_ref, o_ref = blocks
                    else:
                        dy_ref, x_ref, o_ref, a_ref = blocks
                        a_ref[...] = normed(x_ref[...].astype(F32)).astype(BF16)
                    o_ref[...] = dot_nt(dy_ref[...], space[...]).astype(BF16)

                one, out = pl.BlockSpec((big, d), lambda i: (i, 0)), pl.BlockSpec((big, block), lambda i: (i, 0))
                if which:
                    pltpu.emit_pipeline(body, grid=(tokens // big,), in_specs=[one], out_specs=[out])(ref["dy"], ref["early1"])
                else:
                    run_both = pltpu.emit_pipeline(body, grid=(tokens // big,), in_specs=[one, one], out_specs=[out, one])
                    run_both(ref["dy"], ref["x"], ref["early0"], ref["a0"])

            pl.run_scoped(run, pltpu.VMEM((block, d), BF16))

        def gate_up(first, count, acts):
            width, size = count * block, min(256, block)

            def body(scratch, a_ref, s_ref, q_ref, h_ref):
                wg, wu = scratch
                av = a_ref[...]
                for j in range(0, width, size):
                    here = pl.ds(j, size)
                    g, u = dot(av, wg[:, here]), dot(av, wu[:, here])
                    s = sigmoid(g)
                    sl = g * s
                    s_ref[:, here] = sl
                    q_ref[:, here] = u * (s + sl * (1.0 - s))
                    h_ref[:, here] = (sl * u).astype(BF16)

            out = pl.BlockSpec((big, width), lambda i: (i, first // count))
            weights_here = tuple(of[name][first : first + count] for name in ("g0", "u0"))
            stage(body, tokens // big, [pl.BlockSpec((big, d), lambda i: (i, 0))], [out] * 3, ("a0", "silu", "slope", "hidden0"), weights_here, (), acts)

        def down(acts):
            def body(scratch, hidden_ref, x_ref, h_ref, a_ref):
                out = (x_ref[...].astype(F32) + rounded(dot(hidden_ref[...], scratch[0][...]))).astype(BF16)
                h_ref[...] = out
                a_ref[...] = normed(out.astype(F32)).astype(BF16)

            stage(body, tokens // tile, [wide_tile, narrow_tile], [narrow_tile] * 2, ("hidden0", "x", "h1", "a1"), (of["d0"],), (), acts)

        def last_layer():
            size = min(256, block)

            def body(scratch, a_ref, dy_ref, e0_ref, e1_ref, h_ref, dg_ref, du_ref):
                wg, wu, wd = scratch
                av, dyv = a_ref[...], dy_ref[...]
                for q, who in enumerate((at.me, at.mate, at.far, at.far_mate)):
                    for j in range(0, block, size):
                        here = pl.ds(pl.multiple_of(who * block + j, size), size)
                        g, u = dot(av, wg[:, here]), dot(av, wu[:, here])
                        dh = (e0_ref, e1_ref)[q][:, pl.ds(j, size)].astype(F32) if q < 2 else rounded(dot_nt(dyv, wd[here, :]))
                        s = sigmoid(g)
                        sl = g * s
                        h_ref[:, here] = (sl * u).astype(BF16)
                        dg_ref[:, here] = (dh * (u * (s + sl * (1.0 - s)))).astype(BF16)
                        du_ref[:, here] = (dh * sl).astype(BF16)

            specs = [narrow_tile] * 2 + [early_tile] * 2
            arrays = ("a1", "dy", "early0", "early1", "hidden1", "dg1", "du1")
            stage(body, tokens // tile, specs, [wide_tile] * 3, arrays, (of["g1"], of["u1"], of["d1"]))

        at.greet(("mate", "x", "y"))
        move.start(groups[0] + groups[1], "x")
        move.start(of["d1"], "own")
        for group in groups[:-2]:
            move.start(group, "own")
        early(0, ())
        early(1, [(2, over_x, 0)])
        over_x(1)
        over_y(0)
        arrived(0)
        gate_up(0, 1, [(3, over_x, 2), (3, over_y, 1), (7, over_x, 3), (7, over_y, 2)])
        arrived(1)
        gate_up(1, 1, [(3, over_x, 4), (3, over_y, 3), (7, over_x, 5), (7, over_y, 4)])
        arrived(2, 3)
        gate_up(2, 2, [(2, over_x, 6), (2, over_y, 5), (4, over_x, 7), (4, over_y, 6), (6, over_x, 8), (6, over_y, 7)])
        arrived(4, 5)
        down([(0, over_x, 9), (0, over_y, 8), (3, over_x, 10), (4, over_y, 9), (7, over_x, 11), (8, over_y, 10), (12, over_y, 11)])
        arrived(6, 7, 8, 9)
        for n in of["d1"]:
            move.arrived((n,), "straight", "around")
        def first_grads(spaces):
            ahead(("a1",), lambda: grad_out(spaces, "hidden1", "wd1"), other_grads_1, 80)

        def other_grads_1(spaces):
            start(WD1, "mate")
            grad_in(spaces[0], "dg1", "wg1", [(2, WD1, "s")])
            start(WG1, "mate")
            grad_in(spaces[0], "du1", "wu1", [(2, WG1, "s"), (4, WD1, "b")])
            start(WU1, "mate")

        def settled(names, spaces):
            for copy in fetches([of[name] for name in names], spaces):
                copy.wait()
            return spaces

        def other_grads_0():
            def run(space):
                copies = fetches(("a0",), (space,))
                for copy in copies:
                    copy.wait()
                grad_in(space, "dg0", "wg0", [(1, WD0A, "s"), (1, WD0B, "s")])
                start(WG0A, "mate")
                start(WG0B, "mate")
                grad_in(space, "du0", "wu0", [(0, WD0A, "b"), (1, WG0A, "s"), (1, WG0B, "s"), (3, WD0B, "b")])
                start(WU0A, "mate")
                start(WU0B, "mate")

            pl.run_scoped(run, *spaces_for(("a0",)))

        ahead(("dy",), last_layer, first_grads)
        pl.run_scoped(
            lambda *spaces: input_back(
                settled(("g1", "u1"), spaces), "dg1", "du1", "h1", "dy", "dh", [(2, WU1, "s"), (6, WG1, "b"), (14, WU1, "b")]
            ),
            *spaces_for((of["g1"], of["u1"])),
        )
        hidden_back()
        start(WD0A, "mate")
        start(WD0B, "mate")
        late = [(0, WG0A, "b"), (2, WU0A, "s"), (2, WU0B, "s"), (5, WG0B, "b"), (10, WU0A, "b"), (14, WU0B, "b")]
        ahead((of["g0"], of["u0"]), other_grads_0, lambda spaces: input_back(spaces, "dg0", "du0", "x", "dh", "dx", late))
        move.sent(range(len(units)))
        for n in range(len(parts)):
            finish(n, "y")

    results = pl.pallas_call(
        kernel,
        cost_estimate=pl.CostEstimate(flops=34 * tokens * d * ff, bytes_accessed=1 << 30, transcendentals=0),
        compiler_params=pltpu.CompilerParams(vmem_limit_bytes=62 << 20, collective_id=0, has_side_effects=True),
        in_specs=[ANY] * (2 + len(weights)),
        out_specs=[ANY] * len(out_shape),
        out_shape=out_shape,
        scratch_shapes=[
            pltpu.SemaphoreType.DMA((4 * len(parts),)),
            pltpu.SemaphoreType.DMA((4 * len(parts),)),
            pltpu.SemaphoreType.DMA((81,)),
            pltpu.SemaphoreType.DMA((10 * len(parts),)),
            pltpu.SemaphoreType.DMA((len(units), 5)),
            pltpu.SemaphoreType.DMA((len(units), 5)),
        ],
        name="layers",
    )(x, dy, *weights.values())
    dx = results[0]
    sums = {}
    results = results[len(made) + len(units) :]
    for n, part in enumerate(parts):
        group = dict(zip(part_arrays[n], results[5 * n : 5 * n + 5], strict=True))
        sums.setdefault(part.name, []).append((group["b"], group["y"]))
    return dx, sums


def total(*terms):
    return sum(t.astype(F32) for t in terms).astype(BF16)


def solution(mesh):
    def step(x, dy, w_gate, w_up, w_down):
        x, dy = x[0], dy[0]
        weights = {"g": w_gate, "u": w_up, "d": w_down}
        dx, sums = everything(x, dy, weights)

        def out(name):
            return jnp.stack([jnp.concatenate([total(*pair) for pair in sums[name + layer]], 1) for layer in "01"])

        return dx[None], out("wg"), out("wu"), out("wd")

    states, cut = P(("rep", "r", "s"), None, None), P(None, "s", None)
    return jax.shard_map(
        step,
        mesh=mesh,
        in_specs=(states, states) + (cut,) * 3,
        out_specs=(states,) + (P("rep", "s", None),) * 3,
        check_vma=False,
    )
```
